32 devices in a mesh: gy: 8 (over z, x), gx: 4 (over y, core).
Axes of the slice: x: 2, y: 2, z: 4, core: 2. Of those that a mesh axis runs over, the one named last changes fastest.
Arguments:
- imbalance: float32 [4, 1024, 2048], P(None, 'gy', 'gx'), may hold values from -9 to 9
- flow: float32 [2, 4, 1024, 2048], P(None, None, 'gy', 'gx'), may hold values from -3 to 3
- potential: float32 [4, 1024, 2048], P(None, 'gy', 'gx'), may hold values from -5 to 5
- cost: float32 [1024, 2048], P('gy', 'gx'), may hold values from 0.2 to 2
Outputs:
- flow_out: float32 [2, 4, 1024, 2048], P(None, None, 'gy', 'gx')
- potential_out: float32 [4, 1024, 2048], P(None, 'gy', 'gx')
- residual: float32 [4], replicated
The draws below stay inside these ranges and needn't reach their ends.
All inputs are finite; a program needn't handle non-finite values.
Results may differ from the reference program's by a relative error of at most 0.0001.
Values sent between devices are 32-bit elements; how exact they have to be, the bound alone decides.
No kernel may reach another device: no remote copies, remote signals or barrier semaphores. Data moves between devices by JAX's collectives and lax.ppermute only.
A program may use at most 64 MiB of HBM per device.

```python
import math
from functools import partial
import jax
import jax.numpy as jnp
from jax import lax

PAIRS = 4
ITERS = 12
NR = 1024
NC = 2048


def draw_imbalance(key, part):
    row_pos = jnp.arange(NR, dtype=jnp.float32) / max(NR - 1, 1)
    col_pos = jnp.arange(NC, dtype=jnp.float32) / max(NC - 1, 1)
    envelope = 0.25 * (1.0 + 2.0 * row_pos)[:, None] * (1.0 + 2.0 * col_pos)[None, :]
    values = envelope * jnp.clip(jax.random.normal(key, (PAIRS, NR, NC), jnp.float32), -3.5, 3.5)
    return jnp.clip(values, -9.0, 9.0)


def shard_levels(rng, extent, cuts, low, largest):
    loudness = 1.0
    for dim, shards_of in cuts:
        draws = jax.random.uniform(jax.random.fold_in(jax.random.fold_in(rng, 6), dim), (shards_of,), jnp.float32, low / len(cuts), largest / len(cuts))
        loudness = loudness * jnp.repeat(jnp.exp(draws), extent[dim] // shards_of).reshape((-1,) + (1,) * (len(extent) - 1 - dim))
    return loudness


def centred(own_key, dims, spread, bound, pieces=(), held_as=jnp.bfloat16):
    array = jax.random.normal(own_key, dims, jnp.float32) * spread
    if len(pieces) > 0:
        array = shard_levels(own_key, dims, pieces, -0.22, 0.18) * array
    return jnp.clip(array, min=-bound, max=bound).astype(held_as)


def setup_inputs(seed: int = 0) -> dict:
    arg_keys = jax.random.split(jax.random.key(seed), 5)
    imbalance = draw_imbalance(jax.random.fold_in(arg_keys[4], 71), 0)
    flow = centred(arg_keys[1], (2, PAIRS, NR, NC), 0.5, 3.0, ((2, 8), (3, 4)), jnp.float32)
    potential = centred(arg_keys[2], (PAIRS, NR, NC), 1.0, 5.0, ((1, 8), (2, 4)), jnp.float32)
    cost = jnp.clip(jnp.exp(math.log(2.0) - 2.3025851 * jax.random.uniform(arg_keys[3], (NR, NC), jnp.float32) ** shard_levels(arg_keys[3], (NR, NC), ((0, 8), (1, 4)), -0.2, 0.2)), 0.2, 2.0)
    return {"imbalance": imbalance, "flow": flow, "potential": potential, "cost": cost}


initial_step = 0.35
epsilon = 1e-06

def gradient(potential):
    from_below = jnp.concatenate([potential[1:], jnp.zeros_like(potential[:1])], 0)
    from_right = jnp.concatenate([potential[:, 1:], jnp.zeros_like(potential[:, :1])], 1)
    return (from_below - potential, from_right - potential)

def divergence(flow_down, flow_right):
    from_above = jnp.concatenate([jnp.zeros_like(flow_down[:1]), flow_down[:-1]], 0)
    from_left = jnp.concatenate([jnp.zeros_like(flow_right[:, :1]), flow_right[:, :-1]], 1)
    return flow_down - from_above + flow_right - from_left

def shrink(moved_down, moved_right, threshold):
    magnitude = jnp.sqrt(moved_down * moved_down + moved_right * moved_right)
    factor = jnp.maximum(magnitude - threshold, 0.0) / jnp.maximum(magnitude, threshold)
    return (factor * moved_down, factor * moved_right)

def solve_pair(arrays, cost):
    source, flow_down, flow_right, potential = arrays
    primal_rate = jnp.full((), initial_step, jnp.float32)
    dual_rate = jnp.full((), initial_step, jnp.float32)
    spread_old = divergence(flow_down, flow_right)
    for iteration in range(ITERS):
        slope_down, slope_right = gradient(potential)
        new_down, new_right = shrink(flow_down + primal_rate * slope_down, flow_right + primal_rate * slope_right, primal_rate * cost)
        spread_new = divergence(new_down, new_right)
        new_potential = potential + dual_rate * (2.0 * spread_new - spread_old - source)
        if iteration + 1 < ITERS:
            diff_down = new_down - flow_down
            diff_right = new_right - flow_right
            primal_change = jnp.sum(diff_down * diff_down + diff_right * diff_right)
            change = new_potential - potential
            dual_change = jnp.sum(change * change)
            rescale = jnp.sqrt(jnp.sqrt((primal_change + epsilon) / (dual_change + epsilon)))
            primal_rate = primal_rate / rescale
            dual_rate = dual_rate * rescale
        flow_down, flow_right, potential, spread_old = (new_down, new_right, new_potential, spread_new)
    shortfall = spread_old - source
    residual = jnp.sum(shortfall * shortfall) / (NR * NC)
    return (flow_down, flow_right, potential, residual)

def reference(imbalance, flow, potential, cost):
    result_down, result_right, result_potential, residual = lax.map(partial(solve_pair, cost=cost), (imbalance, flow[0], flow[1], potential))
    return (jnp.stack([result_down, result_right]), result_potential, residual)
```

```python
import functools

import jax
import jax.numpy as jnp
from jax import lax
from jax.experimental import pallas as pl
from jax.experimental.pallas import tpu as pltpu
from jax.sharding import PartitionSpec as P

ITERS = 12
initial_step = 0.35
epsilon = 1e-06

DEEP = 12
SLAB = 16
PAD = 8
TOP = PAD + SLAB
LANES = 128
AXES = ("gy", "gx")


def neighbour(value, axis, steps):
    count = lax.axis_size(axis)
    leading, last = (max(0, -steps), min(count, count - steps))
    return lax.ppermute(value, axis, [(source, source + steps) for source in range(leading, last)])


def lane_iota(rows):
    return lax.broadcasted_iota(jnp.int32, (rows, LANES), 1)


def pack_kernel(pairs, imb, flow, pot, cost, up, down, left, right):
    rows, cols = cost.shape
    group = LANES // pairs
    fields = [pot, flow.at[0], flow.at[1], imb]
    for k, field in enumerate(fields):
        for p in range(pairs):
            up[k * pairs + p] = field[p, 0:SLAB, :]
            down[k * pairs + p] = field[p, rows - SLAB : rows, :]
    up[4 * pairs] = cost[0:SLAB, :]
    down[4 * pairs] = cost[rows - SLAB : rows, :]
    lane = lane_iota(rows)
    inner = lane % group
    which = lane // group
    for k in range(5):
        first = jnp.zeros((rows, LANES), jnp.float32)
        last = jnp.zeros((rows, LANES), jnp.float32)
        for p in range(pairs):
            if k < 4:
                head, tail = fields[k][p, :, 0:LANES], fields[k][p, :, cols - LANES : cols]
            else:
                head, tail = cost[:, 0:LANES], cost[:, cols - LANES : cols]
            head = pltpu.roll(head, group * p, 1) if p else head
            shift = (group * (p + 1)) % LANES
            tail = pltpu.roll(tail, shift, 1) if shift else tail
            first = jnp.where((which == p) & (inner < DEEP), head, first)
            last = jnp.where((which == p) & (inner >= group - DEEP), tail, last)
        left[k] = first
        right[k] = last


def own_masks(pairs):
    gy, gx = lax.axis_index("gy"), lax.axis_index("gx")
    above = jnp.where(gy > 0, 1.0, 0.0).astype(jnp.float32)
    below = jnp.where(gy < lax.axis_size("gy") - 1, 1.0, 0.0).astype(jnp.float32)
    inner = lax.broadcasted_iota(jnp.int32, (1, LANES), 1) % (LANES // pairs)
    to_right = (inner < DEEP) & (gx < lax.axis_size("gx") - 1)
    to_left = (inner >= LANES // pairs - DEEP) & (gx > 0)
    sides = jnp.where(to_right | to_left, 1.0, 0.0).astype(jnp.float32)
    return above, below, sides


def assemble_kernel(
    pairs, imb, flow, pot, cost, top, bottom, side, side_top, side_bottom, u, a, b, q, source, price
):
    rows, cols = cost.shape
    per = cols // LANES
    tiles = pairs * per
    end = TOP + rows
    fields = [(u, pot), (a, flow.at[0]), (b, flow.at[1]), (source, imb)]
    for k, (into, field) in enumerate(fields):
        for t in range(tiles + 1):
            into[t, 0:PAD, :] = jnp.zeros((PAD, LANES), jnp.float32)
            into[t, end + SLAB :, :] = jnp.zeros((PAD, LANES), jnp.float32)
        for p in range(pairs):
            for c in range(per):
                t, span = p * per + c, slice(c * LANES, (c + 1) * LANES)
                into[t, PAD:TOP, :] = top[k * pairs + p, :, span]
                into[t, TOP:end, :] = field[p, :, span]
                into[t, end : end + SLAB, :] = bottom[k * pairs + p, :, span]
        into[tiles, PAD:TOP, :] = side_top[k]
        into[tiles, TOP:end, :] = side[k]
        into[tiles, end : end + SLAB, :] = side_bottom[k]
    above, below, sides = own_masks(pairs)
    outside = 1.0 - sides
    for c in range(per):
        span = slice(c * LANES, (c + 1) * LANES)
        price[c, 0:PAD, :] = jnp.ones((PAD, LANES), jnp.float32)
        price[c, end + SLAB :, :] = jnp.ones((PAD, LANES), jnp.float32)
        price[c, PAD:TOP, :] = top[4 * pairs, :, span] + (1.0 - above)
        price[c, TOP:end, :] = cost[:, span]
        price[c, end : end + SLAB, :] = bottom[4 * pairs, :, span] + (1.0 - below)
    price[per, 0:PAD, :] = jnp.ones((PAD, LANES), jnp.float32)
    price[per, end + SLAB :, :] = jnp.ones((PAD, LANES), jnp.float32)
    price[per, PAD:TOP, :] = jnp.where(sides * above > 0.0, side_top[4], 1.0)
    price[per, TOP:end, :] = side[4] + outside
    price[per, end : end + SLAB, :] = jnp.where(sides * below > 0.0, side_bottom[4], 1.0)
    for start, count in chunks(rows, SLAB):
        divergence_rows(pairs, per, start, count, a, b, q)


def chunks(rows, size):
    return [(PAD + k * size, size) for k in range((rows + 2 * SLAB) // size)]


def from_left(pairs, per, b, span):
    group = LANES // pairs
    tiles = pairs * per
    lane = lax.broadcasted_iota(jnp.int32, (span[1], LANES), 1)
    rows = pl.ds(*span)
    side = b[tiles, rows, :]
    moved_side = pltpu.roll(side, 1, 1)
    out = []
    for p in range(pairs):
        shift = (-(group * p + group - 1)) % LANES
        before = pltpu.roll(side, shift, 1) if shift else side
        for c in range(per):
            moved = pltpu.roll(b[p * per + c, rows, :], 1, 1)
            out.append(jnp.where(lane == 0, before, moved))
            before = moved
        landed = pltpu.roll(before, group * p, 1) if p else before
        moved_side = jnp.where(lane == group * p, landed, moved_side)
    return out + [moved_side]


def from_right(pairs, per, u, span):
    group = LANES // pairs
    tiles = pairs * per
    lane = lax.broadcasted_iota(jnp.int32, (span[1], LANES), 1)
    rows = pl.ds(*span)
    side = u[tiles, rows, :]
    moved_side = pltpu.roll(side, LANES - 1, 1)
    out = [None] * tiles
    for p in range(pairs):
        shift = (LANES - 1 - group * p) % LANES
        after = pltpu.roll(side, shift, 1) if shift else side
        for c in reversed(range(per)):
            moved = pltpu.roll(u[p * per + c, rows, :], LANES - 1, 1)
            out[p * per + c] = jnp.where(lane == LANES - 1, after, moved)
            after = moved
        shift = (group * p + group) % LANES
        landed = pltpu.roll(after, shift, 1) if shift else after
        moved_side = jnp.where(lane == group * p + group - 1, landed, moved_side)
    return out + [moved_side]


def divergence_rows(pairs, per, start, count, a, b, q):
    rows, earlier = pl.ds(start, count), pl.ds(start - 1, count)
    left = from_left(pairs, per, b, (start, count))
    for t in range(pairs * per + 1):
        q[t, rows, :] = a[t, rows, :] - a[t, earlier, :] + b[t, rows, :] - left[t]


def folded(value):
    return jnp.sum(value.reshape(-1, 8, LANES), axis=0)


def next_rates(recv, rates):
    total = jnp.sum(recv[...], axis=0, keepdims=True)
    primal = total + epsilon
    dual = pltpu.roll(jnp.broadcast_to(total, (8, LANES)), LANES // 2, 1)[0:1] + epsilon
    rescale = jnp.sqrt(jnp.sqrt(primal / dual))
    return rates[0:1, :] / rescale, rates[1:2, :] * rescale


def spread_rates(pairs, values):
    lane = lax.broadcasted_iota(jnp.int32, (1, LANES), 1)
    each = [jnp.sum(jnp.where(lane == p, values, 0.0)) for p in range(pairs)]
    side = jnp.zeros((1, LANES), jnp.float32)
    for p in range(pairs):
        side = jnp.where(lane // (LANES // pairs) == p, each[p], side)
    return each, side


def lanes_of(parts):
    row = lax.broadcasted_iota(jnp.int32, (8, LANES), 0)
    lane = lax.broadcasted_iota(jnp.int32, (8, LANES), 1)
    matrix = jnp.zeros((8, LANES), jnp.float32)
    where = jnp.zeros((8, LANES), jnp.int32)
    for k, (place, part) in enumerate(parts.items()):
        matrix = jnp.where(row == k, jnp.sum(part, axis=0, keepdims=True), matrix)
        where = jnp.where(row == k, place, where)
    sums = jnp.sum(matrix, axis=1, keepdims=True)
    used = row < len(parts)
    return jnp.sum(jnp.where((lane == where) & used, sums, 0.0), axis=0, keepdims=True)


def primal_rows(pairs, per, start, count, taus, tau_side, masks, price, u, a, b, a_out, b_out, sums):
    rows, later = pl.ds(start, count), pl.ds(start + 1, count)
    right = from_right(pairs, per, u, (start, count))
    row_mask, sides = masks
    for t in range(pairs * per + 1):
        if t < pairs * per:
            rate, cost = taus[t // per], price[t % per, rows, :]
            grad_rate = rate if row_mask is None else rate * row_mask
        else:
            rate, cost = tau_side, price[per, rows, :]
            grad_rate = rate * sides if row_mask is None else rate * sides * row_mask
        here = u[t, rows, :]
        old_down, old_right = a[t, rows, :], b[t, rows, :]
        down = old_down + grad_rate * (u[t, later, :] - here)
        across = old_right + grad_rate * (right[t] - here)
        square = down * down + across * across
        factor = jnp.maximum(1.0 - (rate * cost) * lax.rsqrt(square), 0.0)
        new_down, new_right = factor * down, factor * across
        a_out[t, rows, :] = new_down
        b_out[t, rows, :] = new_right
        if sums is not None and t < pairs * per:
            change_down, change_right = new_down - old_down, new_right - old_right
            p = t // per
            sums[p] = sums[p] + folded(change_down * change_down + change_right * change_right)
    return sums


def iterate_kernel(pairs, rows, recv, rates, price, source, u, a, b, q, u_out, a_out, b_out, q_out, send, rates_out):
    per = price.shape[0] - 1
    tiles = pairs * per
    tau, sigma = next_rates(recv, rates)
    rates_out[0:1, :] = tau
    rates_out[1:2, :] = sigma
    taus, tau_side = spread_rates(pairs, tau)
    sigmas, sigma_side = spread_rates(pairs, sigma)
    above, below, sides = own_masks(pairs)
    primal = [jnp.zeros((8, LANES), jnp.float32)] * pairs
    dual = [jnp.zeros((8, LANES), jnp.float32)] * pairs
    plan = [
        (start, count, above if start < TOP else below if start >= TOP + rows else None)
        for start, count in chunks(rows, SLAB)
    ]
    for start, count, mask in plan:
        found = primal_rows(
            pairs, per, start, count, taus, tau_side, (mask, sides), price, u, a, b, a_out, b_out, primal if mask is None else None
        )
        primal = primal if found is None else found
    for start, count, mask in plan:
        span, earlier = pl.ds(start, count), pl.ds(start - 1, count)
        left = from_left(pairs, per, b_out, (start, count))
        for t in range(tiles + 1):
            rate = sigmas[t // per] if t < tiles else sigma_side * sides
            rate = rate if mask is None else rate * mask
            spread = a_out[t, span, :] - a_out[t, earlier, :] + b_out[t, span, :] - left[t]
            here = u[t, span, :]
            change = rate * (2.0 * spread - q[t, span, :] - source[t, span, :])
            q_out[t, span, :] = spread
            u_out[t, span, :] = here + change
            if mask is None and t < tiles:
                p = t // per
                dual[p] = dual[p] + folded(change * change)
    parts = {p: primal[p] for p in range(pairs)} | {LANES // 2 + p: dual[p] for p in range(pairs)}
    send[...] = jnp.broadcast_to(lanes_of(parts), send.shape)


def closing_kernel(pairs, recv, rates, price, source, u, a, b, q, flow_out, pot_out, send, a_new, b_new):
    per = price.shape[0] - 1
    rows = pot_out.shape[1]
    tiles = pairs * per
    tau, sigma = next_rates(recv, rates)
    taus, tau_side = spread_rates(pairs, tau)
    sigmas, _ = spread_rates(pairs, sigma)
    above, _, sides = own_masks(pairs)
    a_new[:, 0:TOP, :] = jnp.zeros((tiles + 1, TOP, LANES), jnp.float32)
    for start, count in chunks(rows, SLAB)[:-1]:
        mask = above if start < TOP else None
        primal_rows(pairs, per, start, count, taus, tau_side, (mask, sides), price, u, a, b, a_new, b_new, None)
    short = [jnp.zeros((8, LANES), jnp.float32)] * pairs
    for start, count in chunks(rows, SLAB)[1:-1]:
        span, earlier = pl.ds(start, count), pl.ds(start - 1, count)
        left = from_left(pairs, per, b_new, (start, count))
        own = slice(start - TOP, start - TOP + count)
        for t in range(tiles):
            p, c = t // per, t % per
            lanes = slice(c * LANES, (c + 1) * LANES)
            new_down, new_right = a_new[t, span, :], b_new[t, span, :]
            spread = new_down - a_new[t, earlier, :] + new_right - left[t]
            imbalance = source[t, span, :]
            missing = spread - imbalance
            flow_out[0, p, own, lanes] = new_down
            flow_out[1, p, own, lanes] = new_right
            pot_out[p, own, lanes] = u[t, span, :] + sigmas[p] * (2.0 * spread - q[t, span, :] - imbalance)
            short[p] = short[p] + folded(missing * missing)
    send[...] = jnp.broadcast_to(lanes_of({p: short[p] for p in range(pairs)}), send.shape)


def call(kernel, out_shape, operands, aliases=None, scratch=(), limit=24):
    vmem = pl.BlockSpec(memory_space=pltpu.VMEM)
    return pl.pallas_call(
        kernel,
        out_shape=out_shape,
        in_specs=[vmem] * len(operands),
        out_specs=jax.tree.map(lambda _: vmem, out_shape),
        input_output_aliases=aliases or {},
        scratch_shapes=list(scratch),
        compiler_params=pltpu.CompilerParams(vmem_limit_bytes=limit << 20),
    )(*operands)


def shape(*dims):
    return jax.ShapeDtypeStruct(dims, jnp.float32)


def exchange(send):
    return lax.all_to_all(send, AXES, 0, 0, tiled=True)


def local(imbalance, flow, potential, cost):
    pairs, rows, cols = imbalance.shape
    per = cols // LANES
    tiles = pairs * per
    height = rows + 2 * TOP
    devices = lax.axis_size("gy") * lax.axis_size("gx")

    slab, edge = shape(4 * pairs + 1, SLAB, cols), shape(5, rows, LANES)
    up, down, left, right = call(
        functools.partial(pack_kernel, pairs), [slab, slab, edge, edge], [imbalance, flow, potential, cost]
    )
    bottom, top = neighbour(up, "gy", -1), neighbour(down, "gy", 1)
    side = neighbour(left, "gx", -1) + neighbour(right, "gx", 1)
    side_bottom = neighbour(side[:, :SLAB], "gy", -1)
    side_top = neighbour(side[:, rows - SLAB :], "gy", 1)

    field = shape(tiles + 1, height, LANES)
    u, a, b, q, source, price = call(
        functools.partial(assemble_kernel, pairs),
        [field] * 5 + [shape(per + 1, height, LANES)],
        [imbalance, flow, potential, cost, top, bottom, side, side_top, side_bottom],
        limit=32,
    )
    rates = jnp.full((8, LANES), initial_step, jnp.float32)
    recv = jnp.zeros((devices, LANES), jnp.float32)

    def turn(_, carried):
        u, a, b, q, recv, rates = carried
        u, a, b, q, send, rates = call(
            functools.partial(iterate_kernel, pairs, rows),
            [field] * 4 + [shape(devices, LANES), shape(8, LANES)],
            [recv, rates, price, source, u, a, b, q],
            aliases={4: 0, 5: 1, 6: 2, 7: 3, 1: 5},
        )
        return u, a, b, q, exchange(send), rates

    u, a, b, q, recv, rates = lax.fori_loop(0, ITERS - 1, turn, (u, a, b, q, recv, rates))
    new = pltpu.VMEM((tiles + 1, height, LANES), jnp.float32)
    flow_out, pot_out, send = call(
        functools.partial(closing_kernel, pairs),
        [shape(2, pairs, rows, cols), shape(pairs, rows, cols), shape(devices, LANES)],
        [recv, rates, price, source, u, a, b, q],
        scratch=[new, new],
    )
    cells = rows * lax.axis_size("gy") * cols * lax.axis_size("gx")
    residual = jnp.sum(exchange(send), axis=0)[:pairs] / cells
    return flow_out, pot_out, residual


def solution(mesh):
    placed = (P(None, "gy", "gx"), P(None, None, "gy", "gx"), P(None, "gy", "gx"), P("gy", "gx"))
    return jax.shard_map(
        local,
        mesh=mesh,
        in_specs=placed,
        out_specs=(P(None, None, "gy", "gx"), P(None, "gy", "gx"), P()),
        check_vma=False,
    )
```

```python
import functools

import jax
import jax.numpy as jnp
from jax import lax
from jax.experimental import pallas as pl
from jax.experimental.pallas import tpu as pltpu
from jax.sharding import PartitionSpec as P

ITERS = 12
initial_step = 0.35
epsilon = 1e-06

DEPTH = 4
SIDE = ITERS
SLAB = 8
PAD = 8
TOP = PAD + SLAB
LANES = 128
CHUNK = 16
AXES = ("gy", "gx")


def neighbour(value, axis, steps):
    count = lax.axis_size(axis)
    leading, last = (max(0, -steps), min(count, count - steps))
    return lax.ppermute(value, axis, [(source, source + steps) for source in range(leading, last)])


def rolled(value, shift):
    shift = shift % LANES
    return pltpu.roll(value, shift, 1) if shift else value


def pack_kernel(pairs, imb, flow, pot, cost, up, down, left, right, top, bottom, first, last, sems):
    rows, cols = cost.shape
    per, group = cols // LANES, LANES // pairs
    tiles = pairs * per
    fields = [pot, flow.at[0], flow.at[1], imb]
    copies = []

    def fetch(source, target):
        copies.append(pltpu.make_async_copy(source, target, sems.at[len(copies)]))

    for k, field in enumerate(fields):
        fetch(field.at[:, 0:SLAB, :], top.at[pl.ds(k * pairs, pairs)])
        fetch(field.at[:, rows - SLAB : rows, :], bottom.at[pl.ds(k * pairs, pairs)])
    fetch(cost.at[0:SLAB, :], top.at[4 * pairs])
    fetch(cost.at[rows - SLAB : rows, :], bottom.at[4 * pairs])
    slabs = len(copies)
    for k, field in enumerate(fields):
        fetch(field.at[:, :, 0:LANES], first.at[pl.ds(k * pairs, pairs)])
        fetch(field.at[:, :, cols - LANES : cols], last.at[pl.ds(k * pairs, pairs)])
    fetch(cost.at[:, 0:LANES], first.at[4 * pairs])
    fetch(cost.at[:, cols - LANES : cols], last.at[4 * pairs])
    for copy in copies:
        copy.start()
    for copy in copies[:slabs]:
        copy.wait()
    for n in range(4 * pairs + 1):
        for c in range(per):
            span = slice(c * LANES, (c + 1) * LANES)
            up[n * per + c] = top[n, 0:DEPTH, span]
            down[n * per + c] = bottom[n, SLAB - DEPTH : SLAB, span]
    for copy in copies[slabs:]:
        copy.wait()
    count = 32
    lane = lax.broadcasted_iota(jnp.int32, (count, LANES), 1)
    inner, which = lane % group, lane // group
    for k in range(5):
        for start in range(0, rows, count):
            span = slice(start, start + count)
            head = jnp.zeros((count, LANES), jnp.float32)
            tail = jnp.zeros((count, LANES), jnp.float32)
            for p in range(pairs):
                n = min(k * pairs + p, 4 * pairs)
                head = jnp.where((which == p) & (inner < SIDE), rolled(first[n, span, :], group * p), head)
                tail = jnp.where((which == p) & (inner >= group - SIDE), rolled(last[n, span, :], group * (p + 1)), tail)
            left[k, span, :] = head
            right[k, span, :] = tail


def own_masks(pairs):
    gy, gx = lax.axis_index("gy"), lax.axis_index("gx")
    above = jnp.where(gy > 0, 1.0, 0.0).astype(jnp.float32)
    below = jnp.where(gy < lax.axis_size("gy") - 1, 1.0, 0.0).astype(jnp.float32)
    inner = lax.broadcasted_iota(jnp.int32, (1, LANES), 1) % (LANES // pairs)
    to_right = (inner < SIDE) & (gx < lax.axis_size("gx") - 1)
    to_left = (inner >= LANES // pairs - SIDE) & (gx > 0)
    sides = jnp.where(to_right | to_left, 1.0, 0.0).astype(jnp.float32)
    return above, below, sides


def assemble_kernel(
    pairs, imb, flow, pot, cost, top, bottom, side, side_top, side_bottom, u, a, b, q, source, price
):
    rows, cols = cost.shape
    per = cols // LANES
    tiles = pairs * per
    end = TOP + rows
    fields = [(u, pot), (a, flow.at[0]), (b, flow.at[1]), (source, imb)]
    for k, (into, field) in enumerate(fields):
        into[:, 0 : TOP - DEPTH, :] = jnp.zeros((tiles + 1, TOP - DEPTH, LANES), jnp.float32)
        into[:, end + DEPTH :, :] = jnp.zeros((tiles + 1, TOP - DEPTH, LANES), jnp.float32)
        into[0:tiles, TOP - DEPTH : TOP, :] = top[k * tiles : (k + 1) * tiles]
        into[0:tiles, end : end + DEPTH, :] = bottom[k * tiles : (k + 1) * tiles]
        for p in range(pairs):
            for c in range(per):
                into[p * per + c, TOP:end, :] = field[p, :, c * LANES : (c + 1) * LANES]
        into[tiles, TOP - DEPTH : TOP, :] = side_top[k]
        into[tiles, TOP:end, :] = side[k]
        into[tiles, end : end + DEPTH, :] = side_bottom[k]
    above, below, sides = own_masks(pairs)
    price[:, 0 : TOP - DEPTH, :] = jnp.ones((per + 1, TOP - DEPTH, LANES), jnp.float32)
    price[:, end + DEPTH :, :] = jnp.ones((per + 1, TOP - DEPTH, LANES), jnp.float32)
    price[0:per, TOP - DEPTH : TOP, :] = top[4 * tiles :] + (1.0 - above)
    price[0:per, end : end + DEPTH, :] = bottom[4 * tiles :] + (1.0 - below)
    for c in range(per):
        price[c, TOP:end, :] = cost[:, c * LANES : (c + 1) * LANES]
    price[per, TOP - DEPTH : TOP, :] = jnp.where(sides * above > 0.0, side_top[4], 1.0)
    price[per, TOP:end, :] = jnp.where(sides > 0.0, side[4], 1.0)
    price[per, end : end + DEPTH, :] = jnp.where(sides * below > 0.0, side_bottom[4], 1.0)
    q[:, 0:PAD, :] = jnp.zeros((tiles + 1, PAD, LANES), jnp.float32)
    q[:, end + SLAB :, :] = jnp.zeros((tiles + 1, PAD, LANES), jnp.float32)

    def divergence(start, count):
        span, earlier = pl.ds(start, count), pl.ds(start - 1, count)

        def cell(t, p, here, left):
            q[t, span, :] = a[t, span, :] - a[t, earlier, :] + (here - left)

        from_left(pairs, per, b, start, count, cell)

    for start, count in ((PAD, SLAB), (end, SLAB)):
        divergence(start, count)

    def turn(k, carried):
        divergence(TOP + k * CHUNK, CHUNK)
        return carried

    lax.fori_loop(0, rows // CHUNK, turn, 0)


def from_left(pairs, per, b, start, count, cell, closing=False):
    group, tiles = LANES // pairs, pairs * per
    span = pl.ds(start, count)
    lane = lax.broadcasted_iota(jnp.int32, (count, LANES), 1)
    side = b[tiles, span, :]
    moved_side = rolled(side, 1)
    for p in range(pairs):
        before = rolled(side, -(group * p + group - 1))
        for c in range(per):
            here = b[p * per + c, span, :]
            moved = rolled(here, 1)
            cell(p * per + c, p, here, jnp.where(lane == 0, before, moved))
            before = moved
        if not closing:
            moved_side = jnp.where(lane == group * p, rolled(before, group * p), moved_side)
    if not closing:
        cell(tiles, None, side, moved_side)


def from_right(pairs, per, u, start, count, cell):
    group, tiles = LANES // pairs, pairs * per
    span = pl.ds(start, count)
    lane = lax.broadcasted_iota(jnp.int32, (count, LANES), 1)
    side = u[tiles, span, :]
    moved_side = rolled(side, -1)
    for p in range(pairs):
        after = rolled(side, -1 - group * p)
        for c in reversed(range(per)):
            here = u[p * per + c, span, :]
            moved = rolled(here, -1)
            cell(p * per + c, p, here, jnp.where(lane == LANES - 1, after, moved))
            after = moved
        moved_side = jnp.where(lane == group * p + group - 1, rolled(after, group * p + group), moved_side)
    cell(tiles, None, side, moved_side)


def folded(value):
    return jnp.sum(value.reshape(-1, 8, LANES), axis=0)


def next_rates(recv, rates):
    total = jnp.sum(recv[...], axis=0, keepdims=True)
    primal = total + epsilon
    dual = pltpu.roll(jnp.broadcast_to(total, (8, LANES)), LANES // 2, 1)[0:1] + epsilon
    rescale = jnp.sqrt(jnp.sqrt(primal / dual))
    return rates[0:1, :] / rescale, rates[1:2, :] * rescale


def spread_rates(pairs, values):
    lane = lax.broadcasted_iota(jnp.int32, (1, LANES), 1)
    each = [jnp.sum(jnp.where(lane == p, values, 0.0)) for p in range(pairs)]
    side = jnp.zeros((1, LANES), jnp.float32)
    for p in range(pairs):
        side = jnp.where(lane // (LANES // pairs) == p, each[p], side)
    return each, side


def lanes_of(parts):
    row = lax.broadcasted_iota(jnp.int32, (8, LANES), 0)
    lane = lax.broadcasted_iota(jnp.int32, (8, LANES), 1)
    matrix = jnp.zeros((8, LANES), jnp.float32)
    where = jnp.zeros((8, LANES), jnp.int32)
    for k, (place, part) in enumerate(parts.items()):
        matrix = jnp.where(row == k, jnp.sum(part, axis=0, keepdims=True), matrix)
        where = jnp.where(row == k, place, where)
    sums = jnp.sum(matrix, axis=1, keepdims=True)
    used = row < len(parts)
    return jnp.sum(jnp.where((lane == where) & used, sums, 0.0), axis=0, keepdims=True)


def primal_rows(pairs, per, start, count, taus, tau_side, row_mask, sides, price, u, a, b, a_out, b_out, sums):
    span, later = pl.ds(start, count), pl.ds(start + 1, count)
    sums = list(sums)
    side_rate = tau_side * sides if row_mask is None else tau_side * sides * row_mask
    masked = taus if row_mask is None else [tau * row_mask for tau in taus]

    def cell(t, p, here, right):
        rate, grad_rate = (tau_side, side_rate) if p is None else (taus[p], masked[p])
        cost = price[per if p is None else t % per, span, :]
        old_down, old_right = a[t, span, :], b[t, span, :]
        down = old_down + grad_rate * (u[t, later, :] - here)
        across = old_right + grad_rate * (right - here)
        square = down * down + across * across
        factor = jnp.maximum(1.0 - (rate * cost) * lax.rsqrt(square), 0.0)
        new_down, new_right = factor * down, factor * across
        a_out[t, span, :] = new_down
        b_out[t, span, :] = new_right
        if sums and p is not None:
            change_down, change_right = new_down - old_down, new_right - old_right
            sums[p] = sums[p] + folded(change_down * change_down + change_right * change_right)

    from_right(pairs, per, u, start, count, cell)
    return sums


def dual_rows(pairs, per, start, count, sigmas, sigma_side, source, a, b, q, u, q_out, u_out, sums):
    span, earlier = pl.ds(start, count), pl.ds(start - 1, count)
    sums = list(sums)

    def cell(t, p, here, left):
        spread = a[t, span, :] - a[t, earlier, :] + (here - left)
        change = (sigma_side if p is None else sigmas[p]) * (2.0 * spread - q[t, span, :] - source[t, span, :])
        q_out[t, span, :] = spread
        u_out[t, span, :] = u[t, span, :] + change
        if sums and p is not None:
            sums[p] = sums[p] + folded(change * change)

    from_left(pairs, per, b, start, count, cell)
    return sums


def iterate_kernel(pairs, rows, sending, recv, rates, price, source, u, a, b, q, u_out, a_out, b_out, q_out, send, rates_out, *slabs):
    per = price.shape[0] - 1
    tiles = pairs * per
    end, last = TOP + rows, rows // CHUNK - 1
    tau, sigma = next_rates(recv, rates)
    rates_out[0:1, :] = tau
    rates_out[1:2, :] = sigma
    taus, tau_side = spread_rates(pairs, tau)
    sigmas, sigma_side = spread_rates(pairs, sigma)
    above, below, sides = own_masks(pairs)
    for out in (u_out, a_out, b_out, q_out):
        out[:, 0:PAD, :] = jnp.zeros((tiles + 1, PAD, LANES), jnp.float32)
        out[:, end + SLAB :, :] = jnp.zeros((tiles + 1, PAD, LANES), jnp.float32)

    def primal(start, count, mask, sums):
        return primal_rows(pairs, per, start, count, taus, tau_side, mask, sides, price, u, a, b, a_out, b_out, sums)

    def dual(start, count, mask, sums):
        now = sigmas if mask is None else [sigma * mask for sigma in sigmas]
        side_now = sigma_side * sides if mask is None else sigma_side * sides * mask
        return dual_rows(pairs, per, start, count, now, side_now, source, a_out, b_out, q, u, q_out, u_out, sums)

    zeros = [jnp.zeros((8, LANES), jnp.float32)] * pairs
    primal(PAD, SLAB, above, ())
    dual(PAD, SLAB, above, ())
    primals = primal(TOP, CHUNK, None, zeros)

    def turn(k, carried):
        primals, duals = carried
        start = TOP + k * CHUNK
        primals = primal(start, CHUNK, None, primals)
        duals = dual(start - CHUNK, CHUNK, None, duals)
        return tuple(primals), tuple(duals)

    primals, duals = lax.fori_loop(1, last + 1, turn, (tuple(primals), tuple(zeros)))
    primal(end, SLAB, below, ())
    duals = dual(TOP + last * CHUNK, CHUNK, None, duals)
    dual(end, SLAB, below, ())
    parts = {p: primals[p] for p in range(pairs)} | {LANES // 2 + p: duals[p] for p in range(pairs)}
    send[...] = jnp.broadcast_to(lanes_of(parts), send.shape)
    if sending:
        up, down = slabs
        for k, out in enumerate((u_out, a_out, b_out, q_out)):
            up[k] = out[:, TOP : TOP + DEPTH, :]
            down[k] = out[:, end - DEPTH : end, :]


def merge_kernel(rows, recv, top, bottom, u, a, b, q, u_out, a_out, b_out, q_out):
    for k, out in enumerate((u_out, a_out, b_out, q_out)):
        out[:, TOP - DEPTH : TOP, :] = top[k]
        out[:, TOP + rows : TOP + rows + DEPTH, :] = bottom[k]


def closing_kernel(pairs, recv, rates, price, source, u, a, b, q, flow_out, pot_out, send, a_new, b_new):
    per = price.shape[0] - 1
    rows = pot_out.shape[1]
    tau, sigma = next_rates(recv, rates)
    taus, tau_side = spread_rates(pairs, tau)
    sigmas, _ = spread_rates(pairs, sigma)
    above, _, sides = own_masks(pairs)

    def primal(start, count, mask):
        primal_rows(pairs, per, start, count, taus, tau_side, mask, sides, price, u, a, b, a_new, b_new, ())

    def close(k, sums):
        sums = list(sums)
        start = TOP + k * CHUNK
        span, earlier, own = pl.ds(start, CHUNK), pl.ds(start - 1, CHUNK), pl.ds(k * CHUNK, CHUNK)

        def cell(t, p, new_right, left):
            new_down = a_new[t, span, :]
            spread = new_down - a_new[t, earlier, :] + (new_right - left)
            imbalance = source[t, span, :]
            missing = spread - imbalance
            lanes = slice(t % per * LANES, (t % per + 1) * LANES)
            flow_out[0, p, own, lanes] = new_down
            flow_out[1, p, own, lanes] = new_right
            change = sigmas[p] * (2.0 * spread - q[t, span, :] - imbalance)
            pot_out[p, own, lanes] = u[t, span, :] + change
            sums[p] = sums[p] + folded(missing * missing)

        from_left(pairs, per, b_new, start, CHUNK, cell, closing=True)
        return tuple(sums)

    primal(PAD, SLAB, above)
    primal(TOP, CHUNK, None)

    def turn(k, sums):
        primal(TOP + k * CHUNK, CHUNK, None)
        return close(k - 1, sums)

    last = rows // CHUNK - 1
    short = lax.fori_loop(1, last + 1, turn, (jnp.zeros((8, LANES), jnp.float32),) * pairs)
    short = close(last, short)
    send[...] = jnp.broadcast_to(lanes_of({p: short[p] for p in range(pairs)}), send.shape)


def call(kernel, out_shape, operands, aliases=None, scratch=(), limit=8, space=pltpu.VMEM):
    vmem = pl.BlockSpec(memory_space=pltpu.VMEM)
    return pl.pallas_call(
        kernel,
        out_shape=out_shape,
        in_specs=[pl.BlockSpec(memory_space=space)] * len(operands),
        out_specs=[vmem] * len(out_shape),
        input_output_aliases=aliases or {},
        scratch_shapes=list(scratch),
        compiler_params=pltpu.CompilerParams(vmem_limit_bytes=limit << 20),
    )(*operands)


def kept(*dims):
    return pltpu.VMEM(dims, jnp.float32)


def exchange(send):
    return lax.all_to_all(send, AXES, 0, 0, tiled=True)


def local(imbalance, flow, potential, cost):
    pairs, rows, cols = imbalance.shape
    per = cols // LANES
    tiles = pairs * per
    height = rows + 2 * TOP
    devices = lax.axis_size("gy") * lax.axis_size("gx")

    slab, edge = kept(4 * tiles + per, DEPTH, LANES), kept(5, rows, LANES)
    arrays = 4 * pairs + 1
    up, down, left, right = call(
        functools.partial(pack_kernel, pairs),
        [slab, slab, edge, edge],
        [imbalance, flow, potential, cost],
        scratch=[
            kept(arrays, SLAB, cols),
            kept(arrays, SLAB, cols),
            kept(arrays, rows, LANES),
            kept(arrays, rows, LANES),
            pltpu.SemaphoreType.DMA((20,)),
        ],
        space=pltpu.MemorySpace.HBM,
    )
    side = neighbour(left, "gx", -1) + neighbour(right, "gx", 1)
    bottom, top = neighbour(up, "gy", -1), neighbour(down, "gy", 1)
    side_bottom = neighbour(side[:, :DEPTH], "gy", -1)
    side_top = neighbour(side[:, rows - DEPTH :], "gy", 1)

    field = kept(tiles + 1, height, LANES)
    u, a, b, q, source, price = call(
        functools.partial(assemble_kernel, pairs),
        [field] * 5 + [kept(per + 1, height, LANES)],
        [imbalance, flow, potential, cost, top, bottom, side, side_top, side_bottom],
        limit=16,
    )
    rates = jnp.full((8, LANES), initial_step, jnp.float32)
    recv = jnp.zeros((devices, LANES), jnp.float32)
    moving = kept(4, tiles + 1, DEPTH, LANES)
    for k in range(1, ITERS):
        sending = k % DEPTH == 0
        u, a, b, q, send, rates, *slabs = call(
            functools.partial(iterate_kernel, pairs, rows, sending),
            [field] * 4 + [kept(devices, LANES), kept(8, LANES)] + [moving] * 2 * sending,
            [recv, rates, price, source, u, a, b, q],
        )
        if sending:
            bottom, top = neighbour(slabs[0], "gy", -1), neighbour(slabs[1], "gy", 1)
        recv = exchange(send)
        if sending:
            u, a, b, q = call(
                functools.partial(merge_kernel, rows),
                [field] * 4,
                [recv, top, bottom, u, a, b, q],
                aliases={3: 0, 4: 1, 5: 2, 6: 3},
            )
    new = kept(tiles + 1, height, LANES)
    flow_out, pot_out, send = call(
        functools.partial(closing_kernel, pairs),
        [kept(2, pairs, rows, cols), kept(pairs, rows, cols), kept(devices, LANES)],
        [recv, rates, price, source, u, a, b, q],
        scratch=[new, new],
    )
    cells = rows * lax.axis_size("gy") * cols * lax.axis_size("gx")
    residual = jnp.sum(exchange(send), axis=0)[:pairs] / cells
    return flow_out, pot_out, residual


def solution(mesh):
    placed = (P(None, "gy", "gx"), P(None, None, "gy", "gx"), P(None, "gy", "gx"), P("gy", "gx"))
    return jax.shard_map(
        local,
        mesh=mesh,
        in_specs=placed,
        out_specs=(P(None, None, "gy", "gx"), P(None, "gy", "gx"), P()),
        check_vma=False,
    )
```

```python
import functools

import jax
import jax.numpy as jnp
from jax import lax
from jax.experimental import pallas as pl
from jax.experimental.pallas import tpu as pltpu
from jax.sharding import PartitionSpec as P

ITERS = 12
initial_step = 0.35
epsilon = 1e-06

DEPTH = 4
SIDE = ITERS
SLAB = 8
PAD = 8
TOP = PAD + SLAB
LANES = 128
CHUNK = 32
AXES = ("gy", "gx")


def neighbour(value, axis, steps):
    count = lax.axis_size(axis)
    leading, last = (max(0, -steps), min(count, count - steps))
    return lax.ppermute(value, axis, [(source, source + steps) for source in range(leading, last)])


def rolled(value, shift):
    shift = shift % LANES
    return pltpu.roll(value, shift, 1) if shift else value


def edge_kernel(pairs, imb, flow, pot, cost, left, right, up, down, top, bottom, first, last, sems):
    rows, cols = cost.shape
    per, group = cols // LANES, LANES // pairs
    fields = [pot, flow.at[0], flow.at[1], imb]
    copies = []

    def fetch(source, target):
        copies.append(pltpu.make_async_copy(source, target, sems.at[len(copies)]))

    for k, field in enumerate(fields):
        fetch(field.at[:, :, 0:LANES], first.at[pl.ds(k * pairs, pairs)])
        fetch(field.at[:, :, cols - LANES : cols], last.at[pl.ds(k * pairs, pairs)])
    fetch(cost.at[:, 0:LANES], first.at[4 * pairs])
    fetch(cost.at[:, cols - LANES : cols], last.at[4 * pairs])
    sides = len(copies)
    for k, field in enumerate(fields):
        fetch(field.at[:, 0:SLAB, :], top.at[pl.ds(k * pairs, pairs)])
        fetch(field.at[:, rows - SLAB : rows, :], bottom.at[pl.ds(k * pairs, pairs)])
    fetch(cost.at[0:SLAB, :], top.at[4 * pairs])
    fetch(cost.at[rows - SLAB : rows, :], bottom.at[4 * pairs])
    for copy in copies:
        copy.start()
    count = 32
    lane = lax.broadcasted_iota(jnp.int32, (count, LANES), 1)
    inner, which = lane % group, lane // group
    for k in range(5):
        for copy in copies[2 * k : 2 * k + 2]:
            copy.wait()
        for start in range(0, rows, count):
            span = slice(start, start + count)
            head = jnp.zeros((count, LANES), jnp.float32)
            tail = jnp.zeros((count, LANES), jnp.float32)
            for p in range(pairs):
                n = min(k * pairs + p, 4 * pairs)
                head = jnp.where((which == p) & (inner < SIDE), rolled(first[n, span, :], group * p), head)
                tail = jnp.where((which == p) & (inner >= group - SIDE), rolled(last[n, span, :], group * (p + 1)), tail)
            left[k, span, :] = head
            right[k, span, :] = tail
    for copy in copies[sides:]:
        copy.wait()
    for n in range(4 * pairs + 1):
        for c in range(per):
            span = slice(c * LANES, (c + 1) * LANES)
            up[n * per + c] = top[n, 0:DEPTH, span]
            down[n * per + c] = bottom[n, SLAB - DEPTH : SLAB, span]


def slab_kernel(rows, left, right, own_up, own_down, up, down):
    count = own_up.shape[0]
    up[0:count] = own_up[...]
    down[0:count] = own_down[...]
    up[count : count + 5] = left[:, 0:DEPTH, :] + right[:, 0:DEPTH, :]
    down[count : count + 5] = left[:, rows - DEPTH : rows, :] + right[:, rows - DEPTH : rows, :]


def own_masks(pairs):
    gy, gx = lax.axis_index("gy"), lax.axis_index("gx")
    above = jnp.where(gy > 0, 1.0, 0.0).astype(jnp.float32)
    below = jnp.where(gy < lax.axis_size("gy") - 1, 1.0, 0.0).astype(jnp.float32)
    inner = lax.broadcasted_iota(jnp.int32, (1, LANES), 1) % (LANES // pairs)
    to_right = (inner < SIDE) & (gx < lax.axis_size("gx") - 1)
    to_left = (inner >= LANES // pairs - SIDE) & (gx > 0)
    sides = jnp.where(to_right | to_left, 1.0, 0.0).astype(jnp.float32)
    return above, below, sides


def assemble_kernel(pairs, imb, flow, pot, cost, left, right, u, a, b, q, source, price):
    rows, cols = cost.shape
    per = cols // LANES
    tiles = pairs * per
    end = TOP + rows
    fields = [(u, pot), (a, flow.at[0]), (b, flow.at[1]), (source, imb)]
    blank = jnp.zeros((tiles + 1, TOP, LANES), jnp.float32)
    for k, (into, field) in enumerate(fields):
        into[:, 0:TOP, :] = blank
        into[:, end : end + TOP, :] = blank
        for p in range(pairs):
            for c in range(per):
                into[p * per + c, TOP:end, :] = field[p, :, c * LANES : (c + 1) * LANES]
        into[tiles, TOP:end, :] = left[k] + right[k]
    sides = own_masks(pairs)[2]
    price[:, 0:TOP, :] = jnp.ones((per + 1, TOP, LANES), jnp.float32)
    price[:, end : end + TOP, :] = jnp.ones((per + 1, TOP, LANES), jnp.float32)
    for c in range(per):
        price[c, TOP:end, :] = cost[:, c * LANES : (c + 1) * LANES]
    price[per, TOP:end, :] = jnp.where(sides > 0.0, left[4] + right[4], 1.0)
    q[:, 0:TOP, :] = blank
    q[:, end : end + TOP, :] = blank

    def turn(k, carried):
        start_rows(pairs, per, a, b, q, TOP + k * 16, 16)
        return carried

    lax.fori_loop(0, rows // 16, turn, 0)


def start_rows(pairs, per, a, b, q, start, count):
    span, earlier = pl.ds(start, count), pl.ds(start - 1, count)

    def cell(t, p, here, left):
        q[t, span, :] = a[t, span, :] - a[t, earlier, :] + (here - left)

    from_left(pairs, per, b, start, count, cell)


def adopt_kernel(pairs, top, bottom, u, a, b, q, source, price, u_out, a_out, b_out, q_out, source_out, price_out):
    per = price.shape[0] - 1
    tiles = pairs * per
    height = u.shape[1]
    above_rows, below_rows = slice(TOP - DEPTH, TOP), slice(height - TOP, height - TOP + DEPTH)
    above, below, sides = own_masks(pairs)
    for rows, slab, mask in ((above_rows, top, above), (below_rows, bottom, below)):
        for k, out in enumerate((u_out, a_out, b_out, source_out)):
            out[0:tiles, rows, :] = slab[k * tiles : (k + 1) * tiles]
            out[tiles, rows, :] = slab[4 * tiles + per + k]
        price_out[0:per, rows, :] = slab[4 * tiles : 4 * tiles + per] + (1.0 - mask)
        price_out[per, rows, :] = jnp.where(sides * mask > 0.0, slab[4 * tiles + per + 4], 1.0)
    for start in (PAD, TOP, height - TOP):
        start_rows(pairs, per, a_out, b_out, q_out, start, SLAB)


def from_left(pairs, per, b, start, count, cell, closing=False):
    group, tiles = LANES // pairs, pairs * per
    span = pl.ds(start, count)
    lane = lax.broadcasted_iota(jnp.int32, (count, LANES), 1)
    side = b[tiles, span, :]
    moved_side = rolled(side, 1)
    for p in range(pairs):
        before = rolled(side, -(group * p + group - 1))
        for c in range(per):
            here = b[p * per + c, span, :]
            moved = rolled(here, 1)
            cell(p * per + c, p, here, jnp.where(lane == 0, before, moved))
            before = moved
        if not closing:
            moved_side = jnp.where(lane == group * p, rolled(before, group * p), moved_side)
    if not closing:
        cell(tiles, None, side, moved_side)


def from_right(pairs, per, u, start, count, cell):
    group, tiles = LANES // pairs, pairs * per
    span = pl.ds(start, count)
    lane = lax.broadcasted_iota(jnp.int32, (count, LANES), 1)
    side = u[tiles, span, :]
    moved_side = rolled(side, -1)
    for p in range(pairs):
        after = rolled(side, -1 - group * p)
        for c in reversed(range(per)):
            here = u[p * per + c, span, :]
            moved = rolled(here, -1)
            cell(p * per + c, p, here, jnp.where(lane == LANES - 1, after, moved))
            after = moved
        moved_side = jnp.where(lane == group * p + group - 1, rolled(after, group * p + group), moved_side)
    cell(tiles, None, side, moved_side)


def folded(value):
    return jnp.sum(value.reshape(-1, 8, LANES), axis=0)


def next_rates(recv, rates):
    total = jnp.sum(recv[...], axis=0, keepdims=True)
    primal = total + epsilon
    dual = pltpu.roll(jnp.broadcast_to(total, (8, LANES)), LANES // 2, 1)[0:1] + epsilon
    rescale = jnp.sqrt(jnp.sqrt(primal / dual))
    return rates[0:1, :] / rescale, rates[1:2, :] * rescale


def spread_rates(pairs, values):
    lane = lax.broadcasted_iota(jnp.int32, (1, LANES), 1)
    each = [jnp.sum(jnp.where(lane == p, values, 0.0)) for p in range(pairs)]
    side = jnp.zeros((1, LANES), jnp.float32)
    for p in range(pairs):
        side = jnp.where(lane // (LANES // pairs) == p, each[p], side)
    return each, side


def lanes_of(parts):
    row = lax.broadcasted_iota(jnp.int32, (8, LANES), 0)
    lane = lax.broadcasted_iota(jnp.int32, (8, LANES), 1)
    matrix = jnp.zeros((8, LANES), jnp.float32)
    where = jnp.zeros((8, LANES), jnp.int32)
    for k, (place, part) in enumerate(parts.items()):
        matrix = jnp.where(row == k, jnp.sum(part, axis=0, keepdims=True), matrix)
        where = jnp.where(row == k, place, where)
    sums = jnp.sum(matrix, axis=1, keepdims=True)
    used = row < len(parts)
    return jnp.sum(jnp.where((lane == where) & used, sums, 0.0), axis=0, keepdims=True)


def primal_rows(pairs, per, start, count, taus, tau_side, row_mask, sides, price, u, a, b, a_out, b_out, sums):
    span, later = pl.ds(start, count), pl.ds(start + 1, count)
    sums = list(sums)
    side_rate = tau_side * sides if row_mask is None else tau_side * sides * row_mask
    masked = taus if row_mask is None else [tau * row_mask for tau in taus]

    def cell(t, p, here, right):
        rate, grad_rate = (tau_side, side_rate) if p is None else (taus[p], masked[p])
        cost = price[per if p is None else t % per, span, :]
        old_down, old_right = a[t, span, :], b[t, span, :]
        down = old_down + grad_rate * (u[t, later, :] - here)
        across = old_right + grad_rate * (right - here)
        square = down * down + across * across
        factor = jnp.maximum(1.0 - (rate * cost) * lax.rsqrt(square), 0.0)
        new_down, new_right = factor * down, factor * across
        a_out[t, span, :] = new_down
        b_out[t, span, :] = new_right
        if sums and p is not None:
            change_down, change_right = new_down - old_down, new_right - old_right
            sums[p] = sums[p] + folded(change_down * change_down + change_right * change_right)

    from_right(pairs, per, u, start, count, cell)
    return sums


def dual_rows(pairs, per, start, count, sigmas, sigma_side, source, a, b, q, u, q_out, u_out, sums):
    span, earlier = pl.ds(start, count), pl.ds(start - 1, count)
    sums = list(sums)

    def cell(t, p, here, left):
        spread = a[t, span, :] - a[t, earlier, :] + (here - left)
        change = (sigma_side if p is None else sigmas[p]) * (2.0 * spread - q[t, span, :] - source[t, span, :])
        q_out[t, span, :] = spread
        u_out[t, span, :] = u[t, span, :] + change
        if sums and p is not None:
            sums[p] = sums[p] + folded(change * change)

    from_left(pairs, per, b, start, count, cell)
    return sums


def iterate_kernel(pairs, rows, sending, recv, rates, price, source, u, a, b, q, u_out, a_out, b_out, q_out, send, rates_out, *slabs):
    per = price.shape[0] - 1
    tiles = pairs * per
    end, last = TOP + rows, rows // CHUNK - 1
    tau, sigma = next_rates(recv, rates)
    rates_out[0:1, :] = tau
    rates_out[1:2, :] = sigma
    taus, tau_side = spread_rates(pairs, tau)
    sigmas, sigma_side = spread_rates(pairs, sigma)
    above, below, sides = own_masks(pairs)
    for out in (u_out, a_out, b_out, q_out):
        out[:, 0:PAD, :] = jnp.zeros((tiles + 1, PAD, LANES), jnp.float32)
        out[:, end + SLAB :, :] = jnp.zeros((tiles + 1, PAD, LANES), jnp.float32)

    def primal(start, count, mask, sums):
        return primal_rows(pairs, per, start, count, taus, tau_side, mask, sides, price, u, a, b, a_out, b_out, sums)

    def dual(start, count, mask, sums):
        now = sigmas if mask is None else [sigma * mask for sigma in sigmas]
        side_now = sigma_side * sides if mask is None else sigma_side * sides * mask
        return dual_rows(pairs, per, start, count, now, side_now, source, a_out, b_out, q, u, q_out, u_out, sums)

    zeros = [jnp.zeros((8, LANES), jnp.float32)] * pairs
    primal(PAD, SLAB, above, ())
    dual(PAD, SLAB, above, ())
    primals = primal(TOP, CHUNK, None, zeros)

    def turn(k, carried):
        primals, duals = carried
        start = TOP + k * CHUNK
        primals = primal(start, CHUNK, None, primals)
        duals = dual(start - CHUNK, CHUNK, None, duals)
        return tuple(primals), tuple(duals)

    primals, duals = lax.fori_loop(1, last + 1, turn, (tuple(primals), tuple(zeros)))
    primal(end, SLAB, below, ())
    duals = dual(TOP + last * CHUNK, CHUNK, None, duals)
    dual(end, SLAB, below, ())
    parts = {p: primals[p] for p in range(pairs)} | {LANES // 2 + p: duals[p] for p in range(pairs)}
    send[...] = jnp.broadcast_to(lanes_of(parts), send.shape)
    if sending:
        up, down = slabs
        for k, out in enumerate((u_out, a_out, b_out, q_out)):
            up[k] = out[:, TOP : TOP + DEPTH, :]
            down[k] = out[:, end - DEPTH : end, :]


def merge_kernel(rows, recv, top, bottom, u, a, b, q, u_out, a_out, b_out, q_out):
    for k, out in enumerate((u_out, a_out, b_out, q_out)):
        out[:, TOP - DEPTH : TOP, :] = top[k]
        out[:, TOP + rows : TOP + rows + DEPTH, :] = bottom[k]


def closing_kernel(pairs, recv, rates, price, source, u, a, b, q, flow_out, pot_out, send, a_new, b_new):
    per = price.shape[0] - 1
    rows = pot_out.shape[1]
    tau, sigma = next_rates(recv, rates)
    taus, tau_side = spread_rates(pairs, tau)
    sigmas, _ = spread_rates(pairs, sigma)
    above, _, sides = own_masks(pairs)

    def primal(start, count, mask):
        primal_rows(pairs, per, start, count, taus, tau_side, mask, sides, price, u, a, b, a_new, b_new, ())

    def close(k, sums):
        sums = list(sums)
        start = TOP + k * CHUNK
        span, earlier, own = pl.ds(start, CHUNK), pl.ds(start - 1, CHUNK), pl.ds(k * CHUNK, CHUNK)

        def cell(t, p, new_right, left):
            new_down = a_new[t, span, :]
            spread = new_down - a_new[t, earlier, :] + (new_right - left)
            imbalance = source[t, span, :]
            missing = spread - imbalance
            lanes = slice(t % per * LANES, (t % per + 1) * LANES)
            flow_out[0, p, own, lanes] = new_down
            flow_out[1, p, own, lanes] = new_right
            change = sigmas[p] * (2.0 * spread - q[t, span, :] - imbalance)
            pot_out[p, own, lanes] = u[t, span, :] + change
            sums[p] = sums[p] + folded(missing * missing)

        from_left(pairs, per, b_new, start, CHUNK, cell, closing=True)
        return tuple(sums)

    primal(PAD, SLAB, above)
    primal(TOP, CHUNK, None)

    def turn(k, sums):
        primal(TOP + k * CHUNK, CHUNK, None)
        return close(k - 1, sums)

    last = rows // CHUNK - 1
    short = lax.fori_loop(1, last + 1, turn, (jnp.zeros((8, LANES), jnp.float32),) * pairs)
    short = close(last, short)
    send[...] = jnp.broadcast_to(lanes_of({p: short[p] for p in range(pairs)}), send.shape)


def call(kernel, out_shape, operands, aliases=None, scratch=(), limit=8, space=pltpu.VMEM, flops=0):
    vmem = pl.BlockSpec(memory_space=pltpu.VMEM)
    return pl.pallas_call(
        kernel,
        out_shape=out_shape,
        in_specs=[pl.BlockSpec(memory_space=space)] * len(operands),
        out_specs=[vmem] * len(out_shape),
        input_output_aliases=aliases or {},
        scratch_shapes=list(scratch),
        cost_estimate=pl.CostEstimate(flops=flops, bytes_accessed=0, transcendentals=0) if flops else None,
        compiler_params=pltpu.CompilerParams(vmem_limit_bytes=limit << 20),
    )(*operands)


def kept(*dims):
    return pltpu.VMEM(dims, jnp.float32)


def exchange(send):
    return lax.all_to_all(send, AXES, 0, 0, tiled=True)


def local(imbalance, flow, potential, cost):
    pairs, rows, cols = imbalance.shape
    per = cols // LANES
    tiles = pairs * per
    height = rows + 2 * TOP
    devices = lax.axis_size("gy") * lax.axis_size("gx")

    arrays, strips = 4 * pairs + 1, 4 * tiles + per
    edge, slab, moving = kept(5, rows, LANES), kept(strips, DEPTH, LANES), kept(strips + 5, DEPTH, LANES)
    inputs = [imbalance, flow, potential, cost]
    left, right, own_up, own_down = call(
        functools.partial(edge_kernel, pairs),
        [edge, edge, slab, slab],
        [pltpu.with_memory_space_constraint(x, pltpu.MemorySpace.HBM) for x in inputs],
        scratch=[kept(arrays, SLAB, cols)] * 2 + [kept(arrays, rows, LANES)] * 2 + [pltpu.SemaphoreType.DMA((20,))],
        space=pltpu.MemorySpace.HBM,
    )
    left, right = neighbour(left, "gx", -1), neighbour(right, "gx", 1)
    up, down = call(functools.partial(slab_kernel, rows), [moving] * 2, [left, right, own_up, own_down])
    bottom, top = neighbour(up, "gy", -1), neighbour(down, "gy", 1)

    field = kept(tiles + 1, height, LANES)
    fields = [field] * 5 + [kept(per + 1, height, LANES)]
    started = call(functools.partial(assemble_kernel, pairs), fields, inputs + [left, right], flops=40_000_000)
    u, a, b, q, source, price = call(
        functools.partial(adopt_kernel, pairs),
        fields,
        [top, bottom, *started],
        aliases={k + 2: k for k in range(6)},
    )
    rates = jnp.full((8, LANES), initial_step, jnp.float32)
    recv = jnp.zeros((devices, LANES), jnp.float32)
    moving = kept(4, tiles + 1, DEPTH, LANES)
    for k in range(1, ITERS):
        sending = k % DEPTH == 0
        u, a, b, q, send, rates, *slabs = call(
            functools.partial(iterate_kernel, pairs, rows, sending),
            [field] * 4 + [kept(devices, LANES), kept(8, LANES)] + [moving] * 2 * sending,
            [recv, rates, price, source, u, a, b, q],
        )
        if sending:
            bottom, top = neighbour(slabs[0], "gy", -1), neighbour(slabs[1], "gy", 1)
        recv = exchange(send)
        if sending:
            u, a, b, q = call(
                functools.partial(merge_kernel, rows),
                [field] * 4,
                [recv, top, bottom, u, a, b, q],
                aliases={3: 0, 4: 1, 5: 2, 6: 3},
            )
    new = kept(tiles + 1, height, LANES)
    flow_out, pot_out, send = call(
        functools.partial(closing_kernel, pairs),
        [kept(2, pairs, rows, cols), kept(pairs, rows, cols), kept(devices, LANES)],
        [recv, rates, price, source, u, a, b, q],
        scratch=[new, new],
    )
    cells = rows * lax.axis_size("gy") * cols * lax.axis_size("gx")
    residual = jnp.sum(exchange(send), axis=0)[:pairs] / cells
    return flow_out, pot_out, residual


def solution(mesh):
    placed = (P(None, "gy", "gx"), P(None, None, "gy", "gx"), P(None, "gy", "gx"), P("gy", "gx"))
    return jax.shard_map(
        local,
        mesh=mesh,
        in_specs=placed,
        out_specs=(P(None, None, "gy", "gx"), P(None, "gy", "gx"), P()),
        check_vma=False,
    )
```

```python
import functools

import jax
import jax.numpy as jnp
from jax import lax
from jax.experimental import pallas as pl
from jax.experimental.pallas import tpu as pltpu
from jax.sharding import PartitionSpec as P

ITERS = 12
initial_step = 0.35
epsilon = 1e-06

DEPTH = 6
SIDE = ITERS
SLAB = 8
PAD = 8
TOP = PAD + SLAB
LANES = 128
CHUNK = 32
AXES = ("gy", "gx")


def neighbour(value, axis, steps):
    count = lax.axis_size(axis)
    leading, last = (max(0, -steps), min(count, count - steps))
    return lax.ppermute(value, axis, [(source, source + steps) for source in range(leading, last)])


def rolled(value, shift):
    shift = shift % LANES
    return pltpu.roll(value, shift, 1) if shift else value


def edge_kernel(pairs, imb, flow, pot, cost, left, right, up, down, top, bottom, first, last, sems):
    rows, cols = cost.shape
    per, group = cols // LANES, LANES // pairs
    fields = [pot, flow.at[0], flow.at[1], imb]
    copies = []

    def fetch(source, target):
        copies.append(pltpu.make_async_copy(source, target, sems.at[len(copies)]))

    for k, field in enumerate(fields):
        fetch(field.at[:, :, 0:LANES], first.at[pl.ds(k * pairs, pairs)])
        fetch(field.at[:, :, cols - LANES : cols], last.at[pl.ds(k * pairs, pairs)])
    fetch(cost.at[:, 0:LANES], first.at[4 * pairs])
    fetch(cost.at[:, cols - LANES : cols], last.at[4 * pairs])
    sides = len(copies)
    for k, field in enumerate(fields):
        fetch(field.at[:, 0:SLAB, :], top.at[pl.ds(k * pairs, pairs)])
        fetch(field.at[:, rows - SLAB : rows, :], bottom.at[pl.ds(k * pairs, pairs)])
    fetch(cost.at[0:SLAB, :], top.at[4 * pairs])
    fetch(cost.at[rows - SLAB : rows, :], bottom.at[4 * pairs])
    for copy in copies:
        copy.start()
    count = 32
    lane = lax.broadcasted_iota(jnp.int32, (count, LANES), 1)
    inner, which = lane % group, lane // group
    for k in range(5):
        for copy in copies[2 * k : 2 * k + 2]:
            copy.wait()
        for start in range(0, rows, count):
            span = slice(start, start + count)
            head = jnp.zeros((count, LANES), jnp.float32)
            tail = jnp.zeros((count, LANES), jnp.float32)
            for p in range(pairs):
                n = min(k * pairs + p, 4 * pairs)
                head = jnp.where((which == p) & (inner < SIDE), rolled(first[n, span, :], group * p), head)
                tail = jnp.where((which == p) & (inner >= group - SIDE), rolled(last[n, span, :], group * (p + 1)), tail)
            left[k, span, :] = head
            right[k, span, :] = tail
    for copy in copies[sides:]:
        copy.wait()
    for n in range(4 * pairs + 1):
        for c in range(per):
            span = slice(c * LANES, (c + 1) * LANES)
            up[strip(n * per + c), :] = top[n, 0:DEPTH, span]
            down[strip(n * per + c), :] = bottom[n, SLAB - DEPTH : SLAB, span]


def strip(n):
    return slice(n * DEPTH, (n + 1) * DEPTH)


def strips(count):
    return kept(-(-count * DEPTH // 8) * 8, LANES)


def slab_kernel(rows, count, left, right, own_up, own_down, up, down):
    up[0 : count * DEPTH, :] = own_up[0 : count * DEPTH, :]
    down[0 : count * DEPTH, :] = own_down[0 : count * DEPTH, :]
    for k in range(5):
        up[strip(count + k), :] = left[k, 0:DEPTH, :] + right[k, 0:DEPTH, :]
        down[strip(count + k), :] = left[k, rows - DEPTH : rows, :] + right[k, rows - DEPTH : rows, :]


def own_masks(pairs):
    gy, gx = lax.axis_index("gy"), lax.axis_index("gx")
    above = jnp.where(gy > 0, 1.0, 0.0).astype(jnp.float32)
    below = jnp.where(gy < lax.axis_size("gy") - 1, 1.0, 0.0).astype(jnp.float32)
    inner = lax.broadcasted_iota(jnp.int32, (1, LANES), 1) % (LANES // pairs)
    to_right = (inner < SIDE) & (gx < lax.axis_size("gx") - 1)
    to_left = (inner >= LANES // pairs - SIDE) & (gx > 0)
    sides = jnp.where(to_right | to_left, 1.0, 0.0).astype(jnp.float32)
    return above, below, sides


def assemble_kernel(pairs, imb, flow, pot, cost, left, right, u, a, b, source, price):
    rows, cols = cost.shape
    per = cols // LANES
    tiles = pairs * per
    end = TOP + rows
    fields = [(u, pot), (a, flow.at[0]), (b, flow.at[1]), (source, imb)]
    blank = jnp.zeros((tiles + 1, TOP, LANES), jnp.float32)
    for k, (into, field) in enumerate(fields):
        into[:, 0:TOP, :] = blank
        into[:, end : end + TOP, :] = blank
        for p in range(pairs):
            for c in range(per):
                into[p * per + c, TOP:end, :] = field[p, :, c * LANES : (c + 1) * LANES]
        into[tiles, TOP:end, :] = left[k] + right[k]
    sides = own_masks(pairs)[2]
    price[:, 0:TOP, :] = jnp.ones((per + 1, TOP, LANES), jnp.float32)
    price[:, end : end + TOP, :] = jnp.ones((per + 1, TOP, LANES), jnp.float32)
    for c in range(per):
        price[c, TOP:end, :] = cost[:, c * LANES : (c + 1) * LANES]
    price[per, TOP:end, :] = jnp.where(sides > 0.0, left[4] + right[4], 1.0)


def adopt_kernel(pairs, rows, top, bottom, u, a, b, source, price, u_out, a_out, b_out, source_out, price_out):
    per = price.shape[0] - 1
    tiles = pairs * per
    end, count = TOP + rows, 4 * tiles + per
    above, below, sides = own_masks(pairs)
    for span, slab, mask in ((slice(TOP - DEPTH, TOP), top, above), (slice(end, end + DEPTH), bottom, below)):
        for k, out in enumerate((u_out, a_out, b_out, source_out)):
            for t in range(tiles):
                out[t, span, :] = slab[strip(k * tiles + t), :]
            out[tiles, span, :] = slab[strip(count + k), :]
        for c in range(per):
            price_out[c, span, :] = slab[strip(4 * tiles + c), :] + (1.0 - mask)
        price_out[per, span, :] = jnp.where(sides * mask > 0.0, slab[strip(count + 4), :], 1.0)


def from_left(pairs, per, b, start, count, cell, closing=False):
    group, tiles = LANES // pairs, pairs * per
    span = pl.ds(start, count)
    lane = lax.broadcasted_iota(jnp.int32, (count, LANES), 1)
    side = b[tiles, span, :]
    moved_side = rolled(side, 1)
    for p in range(pairs):
        before = rolled(side, -(group * p + group - 1))
        for c in range(per):
            here = b[p * per + c, span, :]
            moved = rolled(here, 1)
            cell(p * per + c, p, here, jnp.where(lane == 0, before, moved))
            before = moved
        if not closing:
            moved_side = jnp.where(lane == group * p, rolled(before, group * p), moved_side)
    if not closing:
        cell(tiles, None, side, moved_side)


def from_right(pairs, per, u, start, count, cell):
    group, tiles = LANES // pairs, pairs * per
    span = pl.ds(start, count)
    lane = lax.broadcasted_iota(jnp.int32, (count, LANES), 1)
    side = u[tiles, span, :]
    moved_side = rolled(side, -1)
    for p in range(pairs):
        after = rolled(side, -1 - group * p)
        for c in reversed(range(per)):
            here = u[p * per + c, span, :]
            moved = rolled(here, -1)
            cell(p * per + c, p, here, jnp.where(lane == LANES - 1, after, moved))
            after = moved
        moved_side = jnp.where(lane == group * p + group - 1, rolled(after, group * p + group), moved_side)
    cell(tiles, None, side, moved_side)


def folded(value):
    return jnp.sum(value.reshape(-1, 8, LANES), axis=0)


def same_parity(value):
    value = value + pltpu.roll(value, 2, 0)
    return value + pltpu.roll(value, 4, 0)


def next_rates(recv, rates):
    total = same_parity(folded(recv[...])) + epsilon
    ratio = total / pltpu.roll(total, 1, 0)
    return rates[...] * lax.rsqrt(lax.rsqrt(ratio))


def spread_rates(pairs, rates):
    group = lax.broadcasted_iota(jnp.int32, (8, LANES), 1) // (LANES // pairs)
    each = [jnp.max(jnp.where(group == p, rates, 0.0), axis=1, keepdims=True) for p in range(pairs)]
    each = [jnp.broadcast_to(value, (8, LANES)) for value in each]
    return [v[1:2] for v in each], rates[1:2], [v[0:1] for v in each], rates[0:1]


def sums_to_send(pairs, even, odd):
    row = lax.broadcasted_iota(jnp.int32, (8, LANES), 0)
    group = lax.broadcasted_iota(jnp.int32, (8, LANES), 1) // (LANES // pairs)
    matrix = jnp.zeros((8, LANES), jnp.float32)
    for p in range(pairs):
        for k, part in ((2 * p, even[p]), (2 * p + 1, odd[p])):
            if part is not None:
                matrix = jnp.where(row == k, jnp.sum(part, axis=0, keepdims=True), matrix)
    sums = jnp.sum(matrix, axis=1, keepdims=True)
    return same_parity(jnp.where(group == row // 2, sums, 0.0))


def put_sums(send, sums):
    for start in range(0, send.shape[0], 8):
        send[start : start + 8, :] = sums


def primal_rows(pairs, per, start, count, taus, tau_side, row_mask, sides, price, u, a, b, a_out, b_out, a_far, b_far, sums):
    span, later = pl.ds(start, count), pl.ds(start + 1, count)
    sums = list(sums)
    side_rate = tau_side * sides if row_mask is None else tau_side * sides * row_mask
    masked = taus if row_mask is None else [tau * row_mask for tau in taus]

    def cell(t, p, here, right):
        rate, grad_rate = (tau_side, side_rate) if p is None else (taus[p], masked[p])
        cost = price[per if p is None else t % per, span, :]
        old_down, old_right = a[t, span, :], b[t, span, :]
        down = old_down + grad_rate * (u[t, later, :] - here)
        across = old_right + grad_rate * (right - here)
        square = down * down + across * across
        factor = jnp.maximum(1.0 - (rate * cost) * lax.rsqrt(square), 0.0)
        new_down, new_right = factor * down, factor * across
        a_out[t, span, :] = new_down
        b_out[t, span, :] = new_right
        change_down, change_right = new_down - old_down, new_right - old_right
        a_far[t, span, :] = new_down + change_down
        b_far[t, span, :] = new_right + change_right
        if sums and p is not None:
            sums[p] = sums[p] + folded(change_down * change_down + change_right * change_right)

    from_right(pairs, per, u, start, count, cell)
    return sums


def dual_rows(pairs, per, start, count, sigmas, sigma_side, source, a_far, b_far, u, u_out, sums):
    span, earlier = pl.ds(start, count), pl.ds(start - 1, count)
    sums = list(sums)

    def cell(t, p, here, left):
        spread = a_far[t, span, :] - a_far[t, earlier, :] + (here - left)
        change = (sigma_side if p is None else sigmas[p]) * (spread - source[t, span, :])
        u_out[t, span, :] = u[t, span, :] + change
        if sums and p is not None:
            sums[p] = sums[p] + folded(change * change)

    from_left(pairs, per, b_far, start, count, cell)
    return sums


def iterate_kernel(pairs, rows, sending, recv, rates, price, source, u, a, b, u_out, a_out, b_out, send, rates_out, *rest):
    slabs, (a_far, b_far) = rest[:-2], rest[-2:]
    per = price.shape[0] - 1
    tiles = pairs * per
    end, last = TOP + rows, rows // CHUNK - 1
    rates_now = next_rates(recv, rates)
    rates_out[...] = rates_now
    taus, tau_side, sigmas, sigma_side = spread_rates(pairs, rates_now)
    above, below, sides = own_masks(pairs)
    a_far[:, 0:PAD, :] = jnp.zeros((tiles + 1, PAD, LANES), jnp.float32)
    u_out[:, end + SLAB : end + TOP, :] = jnp.zeros((tiles + 1, PAD, LANES), jnp.float32)

    def primal(start, count, mask, sums):
        return primal_rows(
            pairs, per, start, count, taus, tau_side, mask, sides, price, u, a, b, a_out, b_out, a_far, b_far, sums
        )

    def dual(start, count, mask, sums):
        now = sigmas if mask is None else [sigma * mask for sigma in sigmas]
        side_now = sigma_side * sides if mask is None else sigma_side * sides * mask
        return dual_rows(pairs, per, start, count, now, side_now, source, a_far, b_far, u, u_out, sums)

    zeros = [jnp.zeros((8, LANES), jnp.float32)] * pairs
    primal(PAD, SLAB, above, ())
    dual(PAD, SLAB, above, ())
    primals = primal(TOP, CHUNK, None, zeros)

    def turn(k, carried):
        primals, duals = carried
        start = TOP + k * CHUNK
        primals = primal(start, CHUNK, None, primals)
        duals = dual(start - CHUNK, CHUNK, None, duals)
        return tuple(primals), tuple(duals)

    primals, duals = lax.fori_loop(1, last + 1, turn, (tuple(primals), tuple(zeros)))
    primal(end, SLAB, below, ())
    duals = dual(TOP + last * CHUNK, CHUNK, None, duals)
    dual(end, SLAB, below, ())
    put_sums(send, sums_to_send(pairs, primals, duals))
    if sending:
        up, down = slabs
        for k, out in enumerate((u_out, a_out, b_out)):
            for t in range(tiles + 1):
                up[strip(k * (tiles + 1) + t), :] = out[t, TOP : TOP + DEPTH, :]
                down[strip(k * (tiles + 1) + t), :] = out[t, end - DEPTH : end, :]


def merge_kernel(rows, recv, top, bottom, u, a, b, u_out, a_out, b_out):
    tiles = u.shape[0]
    for k, out in enumerate((u_out, a_out, b_out)):
        for t in range(tiles):
            out[t, TOP - DEPTH : TOP, :] = top[strip(k * tiles + t), :]
            out[t, TOP + rows : TOP + rows + DEPTH, :] = bottom[strip(k * tiles + t), :]


def closing_kernel(
    pairs, recv, rates, price, source, u, a, b, flow_out, pot_out, send, a_new, b_new, a_far, b_far
):
    per = price.shape[0] - 1
    rows = pot_out.shape[1]
    taus, tau_side, sigmas, _ = spread_rates(pairs, next_rates(recv, rates))
    above, _, sides = own_masks(pairs)

    def primal(start, count, mask):
        primal_rows(
            pairs, per, start, count, taus, tau_side, mask, sides, price, u, a, b, a_new, b_new, a_far, b_far, ()
        )

    def close(k, sums):
        sums = list(sums)
        start = TOP + k * CHUNK
        span, earlier, own = pl.ds(start, CHUNK), pl.ds(start - 1, CHUNK), pl.ds(k * CHUNK, CHUNK)

        def lanes(t):
            return slice(t % per * LANES, (t % per + 1) * LANES)

        def shortfall(t, p, here, left):
            down = a_new[t, span, :]
            missing = down - a_new[t, earlier, :] + (here - left) - source[t, span, :]
            flow_out[0, p, own, lanes(t)] = down
            flow_out[1, p, own, lanes(t)] = here
            sums[p] = sums[p] + folded(missing * missing)

        def rise(t, p, here, left):
            spread = a_far[t, span, :] - a_far[t, earlier, :] + (here - left)
            pot_out[p, own, lanes(t)] = u[t, span, :] + sigmas[p] * (spread - source[t, span, :])

        from_left(pairs, per, b_new, start, CHUNK, shortfall, closing=True)
        from_left(pairs, per, b_far, start, CHUNK, rise, closing=True)
        return tuple(sums)

    primal(PAD, SLAB, above)
    primal(TOP, CHUNK, None)

    def turn(k, sums):
        primal(TOP + k * CHUNK, CHUNK, None)
        return close(k - 1, sums)

    last = rows // CHUNK - 1
    short = lax.fori_loop(1, last + 1, turn, (jnp.zeros((8, LANES), jnp.float32),) * pairs)
    short = close(last, short)
    put_sums(send, sums_to_send(pairs, short, [None] * pairs))


def call(kernel, out_shape, operands, aliases=None, scratch=(), limit=8, space=pltpu.VMEM, flops=0):
    vmem = pl.BlockSpec(memory_space=pltpu.VMEM)
    return pl.pallas_call(
        kernel,
        out_shape=out_shape,
        in_specs=[pl.BlockSpec(memory_space=space)] * len(operands),
        out_specs=[vmem] * len(out_shape),
        input_output_aliases=aliases or {},
        scratch_shapes=list(scratch),
        cost_estimate=pl.CostEstimate(flops=flops, bytes_accessed=0, transcendentals=0) if flops else None,
        compiler_params=pltpu.CompilerParams(vmem_limit_bytes=limit << 20),
    )(*operands)


def kept(*dims):
    return pltpu.VMEM(dims, jnp.float32)


def exchange(send):
    return lax.all_to_all(send, AXES, 0, 0, tiled=True)


def local(imbalance, flow, potential, cost):
    pairs, rows, cols = imbalance.shape
    per = cols // LANES
    tiles = pairs * per
    height = rows + 2 * TOP
    devices = lax.axis_size("gy") * lax.axis_size("gx")

    arrays, count = 4 * pairs + 1, 4 * tiles + per
    edge = kept(5, rows, LANES)
    inputs = [imbalance, flow, potential, cost]
    left, right, own_up, own_down = call(
        functools.partial(edge_kernel, pairs),
        [edge, edge, strips(count), strips(count)],
        [pltpu.with_memory_space_constraint(x, pltpu.MemorySpace.HBM) for x in inputs],
        scratch=[kept(arrays, SLAB, cols)] * 2 + [kept(arrays, rows, LANES)] * 2 + [pltpu.SemaphoreType.DMA((20,))],
        space=pltpu.MemorySpace.HBM,
    )
    left, right = neighbour(left, "gx", -1), neighbour(right, "gx", 1)
    up, down = call(
        functools.partial(slab_kernel, rows, count), [strips(count + 5)] * 2, [left, right, own_up, own_down]
    )
    bottom, top = neighbour(up, "gy", -1), neighbour(down, "gy", 1)

    field = kept(tiles + 1, height, LANES)
    fields = [field] * 4 + [kept(per + 1, height, LANES)]
    started = call(functools.partial(assemble_kernel, pairs), fields, inputs + [left, right], flops=40_000_000)
    u, a, b, source, price = call(
        functools.partial(adopt_kernel, pairs, rows),
        fields,
        [top, bottom, *started],
        aliases={k + 2: k for k in range(5)},
    )
    rates = jnp.full((8, LANES), initial_step, jnp.float32)
    recv = jnp.zeros((2 * devices, LANES), jnp.float32)
    for k in range(1, ITERS):
        sending = k % DEPTH == 0
        u, a, b, send, rates, *slabs = call(
            functools.partial(iterate_kernel, pairs, rows, sending),
            [field] * 3 + [kept(2 * devices, LANES), kept(8, LANES)] + [strips(3 * (tiles + 1))] * 2 * sending,
            [recv, rates, price, source, u, a, b],
            scratch=[field] * 2,
        )
        if sending:
            bottom, top = neighbour(slabs[0], "gy", -1), neighbour(slabs[1], "gy", 1)
        recv = exchange(send)
        if sending:
            u, a, b = call(
                functools.partial(merge_kernel, rows),
                [field] * 3,
                [recv, top, bottom, u, a, b],
                aliases={3: 0, 4: 1, 5: 2},
            )
    flow_out, pot_out, send = call(
        functools.partial(closing_kernel, pairs),
        [kept(2, pairs, rows, cols), kept(pairs, rows, cols), kept(2 * devices, LANES)],
        [recv, rates, price, source, u, a, b],
        scratch=[field] * 4,
        limit=12,
    )
    cells = rows * lax.axis_size("gy") * cols * lax.axis_size("gx")
    residual = jnp.sum(exchange(send), axis=0)[:: LANES // pairs] / cells
    return flow_out, pot_out, residual


def solution(mesh):
    placed = (P(None, "gy", "gx"), P(None, None, "gy", "gx"), P(None, "gy", "gx"), P("gy", "gx"))
    return jax.shard_map(
        local,
        mesh=mesh,
        in_specs=placed,
        out_specs=(P(None, None, "gy", "gx"), P(None, "gy", "gx"), P()),
        check_vma=False,
    )
```

```python
import functools

import jax
import jax.numpy as jnp
from jax import lax
from jax.experimental import pallas as pl
from jax.experimental.pallas import tpu as pltpu
from jax.sharding import PartitionSpec as P

ITERS = 12
initial_step = 0.35
epsilon = 1e-06

DEPTH = 6
SIDE = ITERS
SLAB = 8
PAD = 8
TOP = PAD + SLAB
LANES = 128
CLOSING_CHUNK = 64
CHUNK = 32
AXES = ("gy", "gx")


def neighbour(value, axis, steps):
    count = lax.axis_size(axis)
    leading, last = (max(0, -steps), min(count, count - steps))
    return lax.ppermute(value, axis, [(source, source + steps) for source in range(leading, last)])


def rolled(value, shift):
    shift = shift % LANES
    return pltpu.roll(value, shift, 1) if shift else value


def edge_columns_kernel(pairs, imb, flow, pot, cost, left, right, first, last, sems):
    rows, cols = cost.shape
    group = LANES // pairs
    fields = [pot, flow.at[0], flow.at[1], imb]
    copies = []

    def fetch(source, target):
        copies.append(pltpu.make_async_copy(source, target, sems.at[len(copies)]))

    for k, field in enumerate(fields):
        fetch(field.at[:, :, 0:LANES], first.at[pl.ds(k * pairs, pairs)])
        fetch(field.at[:, :, cols - LANES : cols], last.at[pl.ds(k * pairs, pairs)])
    fetch(cost.at[:, 0:LANES], first.at[4 * pairs])
    fetch(cost.at[:, cols - LANES : cols], last.at[4 * pairs])
    for copy in copies:
        copy.start()
    count = 32
    lane = lax.broadcasted_iota(jnp.int32, (count, LANES), 1)
    inner, which = lane % group, lane // group
    for k in range(5):
        for copy in copies[2 * k : 2 * k + 2]:
            copy.wait()
        for start in range(0, rows, count):
            span = slice(start, start + count)
            head = jnp.zeros((count, LANES), jnp.float32)
            tail = jnp.zeros((count, LANES), jnp.float32)
            for p in range(pairs):
                n = min(k * pairs + p, 4 * pairs)
                head = jnp.where((which == p) & (inner < SIDE), rolled(first[n, span, :], group * p), head)
                tail = jnp.where((which == p) & (inner >= group - SIDE), rolled(last[n, span, :], group * (p + 1)), tail)
            left[k, span, :] = head
            right[k, span, :] = tail


def edge_rows_kernel(pairs, imb, flow, pot, cost, up, down, top, bottom, sems):
    rows, cols = cost.shape
    per = cols // LANES
    copies = []

    def fetch(source, target):
        copies.append(pltpu.make_async_copy(source, target, sems.at[len(copies)]))

    for k, field in enumerate([pot, flow.at[0], flow.at[1], imb]):
        fetch(field.at[:, 0:SLAB, :], top.at[pl.ds(k * pairs, pairs)])
        fetch(field.at[:, rows - SLAB : rows, :], bottom.at[pl.ds(k * pairs, pairs)])
    fetch(cost.at[0:SLAB, :], top.at[4 * pairs])
    fetch(cost.at[rows - SLAB : rows, :], bottom.at[4 * pairs])
    for copy in copies:
        copy.start()
    for copy in copies:
        copy.wait()
    for n in range(4 * pairs + 1):
        for c in range(per):
            span = slice(c * LANES, (c + 1) * LANES)
            up[strip(n * per + c), :] = top[n, 0:DEPTH, span]
            down[strip(n * per + c), :] = bottom[n, SLAB - DEPTH : SLAB, span]


def strip(n):
    return slice(n * DEPTH, (n + 1) * DEPTH)


def strips(count):
    return kept(-(-count * DEPTH // 8) * 8, LANES)


def slab_kernel(rows, count, left, right, own_up, own_down, up, down):
    up[0 : count * DEPTH, :] = own_up[0 : count * DEPTH, :]
    down[0 : count * DEPTH, :] = own_down[0 : count * DEPTH, :]
    for k in range(5):
        up[strip(count + k), :] = left[k, 0:DEPTH, :] + right[k, 0:DEPTH, :]
        down[strip(count + k), :] = left[k, rows - DEPTH : rows, :] + right[k, rows - DEPTH : rows, :]


def own_masks(pairs):
    gy, gx = lax.axis_index("gy"), lax.axis_index("gx")
    above = jnp.where(gy > 0, 1.0, 0.0).astype(jnp.float32)
    below = jnp.where(gy < lax.axis_size("gy") - 1, 1.0, 0.0).astype(jnp.float32)
    inner = lax.broadcasted_iota(jnp.int32, (1, LANES), 1) % (LANES // pairs)
    to_right = (inner < SIDE) & (gx < lax.axis_size("gx") - 1)
    to_left = (inner >= LANES // pairs - SIDE) & (gx > 0)
    sides = jnp.where(to_right | to_left, 1.0, 0.0).astype(jnp.float32)
    return above, below, sides


def assemble_kernel(pairs, imb, flow, pot, cost, left, right, u, a, b, source, price):
    rows, cols = cost.shape
    per = cols // LANES
    tiles = pairs * per
    end = TOP + rows
    fields = [(u, pot), (a, flow.at[0]), (b, flow.at[1]), (source, imb)]
    blank = jnp.zeros((tiles + 1, TOP, LANES), jnp.float32)
    for k, (into, field) in enumerate(fields):
        into[:, 0:TOP, :] = blank
        into[:, end : end + TOP, :] = blank
        for p in range(pairs):
            for c in range(per):
                into[p * per + c, TOP:end, :] = field[p, :, c * LANES : (c + 1) * LANES]
        into[tiles, TOP:end, :] = left[k] + right[k]
    sides = own_masks(pairs)[2]
    price[:, 0:TOP, :] = jnp.ones((per + 1, TOP, LANES), jnp.float32)
    price[:, end : end + TOP, :] = jnp.ones((per + 1, TOP, LANES), jnp.float32)
    for c in range(per):
        price[c, TOP:end, :] = cost[:, c * LANES : (c + 1) * LANES]
    price[per, TOP:end, :] = jnp.where(sides > 0.0, left[4] + right[4], 1.0)


def adopt_kernel(pairs, rows, early_sums, top, bottom, u, a, b, source, price, u_out, a_out, b_out, source_out, price_out):
    per = price.shape[0] - 1
    tiles = pairs * per
    end, count = TOP + rows, 4 * tiles + per
    above, below, sides = own_masks(pairs)
    for span, slab, mask in ((slice(TOP - DEPTH, TOP), top, above), (slice(end, end + DEPTH), bottom, below)):
        for k, out in enumerate((u_out, a_out, b_out, source_out)):
            for t in range(tiles):
                out[t, span, :] = slab[strip(k * tiles + t), :]
            out[tiles, span, :] = slab[strip(count + k), :]
        for c in range(per):
            price_out[c, span, :] = slab[strip(4 * tiles + c), :] + (1.0 - mask)
        price_out[per, span, :] = jnp.where(sides * mask > 0.0, slab[strip(count + 4), :], 1.0)


def from_left(pairs, per, b, start, count, cell, closing=False):
    group, tiles = LANES // pairs, pairs * per
    span = pl.ds(start, count)
    lane = lax.broadcasted_iota(jnp.int32, (count, LANES), 1)
    side = b[tiles, span, :]
    moved_side = rolled(side, 1)
    for p in range(pairs):
        before = rolled(side, -(group * p + group - 1))
        for c in range(per):
            here = b[p * per + c, span, :]
            moved = rolled(here, 1)
            cell(p * per + c, p, here, jnp.where(lane == 0, before, moved))
            before = moved
        if not closing:
            moved_side = jnp.where(lane == group * p, rolled(before, group * p), moved_side)
    if not closing:
        cell(tiles, None, side, moved_side)


def from_right(pairs, per, u, start, count, cell):
    group, tiles = LANES // pairs, pairs * per
    span = pl.ds(start, count)
    lane = lax.broadcasted_iota(jnp.int32, (count, LANES), 1)
    side = u[tiles, span, :]
    moved_side = rolled(side, -1)
    for p in range(pairs):
        after = rolled(side, -1 - group * p)
        for c in reversed(range(per)):
            here = u[p * per + c, span, :]
            moved = rolled(here, -1)
            cell(p * per + c, p, here, jnp.where(lane == LANES - 1, after, moved))
            after = moved
        moved_side = jnp.where(lane == group * p + group - 1, rolled(after, group * p + group), moved_side)
    cell(tiles, None, side, moved_side)


def folded(value):
    return jnp.sum(value.reshape(-1, 8, LANES), axis=0)


def same_parity(value):
    value = value + pltpu.roll(value, 2, 0)
    return value + pltpu.roll(value, 4, 0)


def next_rates(recv, rates):
    total = same_parity(folded(recv[...])) + epsilon
    ratio = total / pltpu.roll(total, 1, 0)
    return rates[...] * lax.rsqrt(lax.rsqrt(ratio))


def spread_rates(pairs, rates):
    group = lax.broadcasted_iota(jnp.int32, (8, LANES), 1) // (LANES // pairs)
    each = [jnp.max(jnp.where(group == p, rates, 0.0), axis=1, keepdims=True) for p in range(pairs)]
    each = [jnp.broadcast_to(value, (8, LANES)) for value in each]
    return [v[1:2] for v in each], rates[1:2], [v[0:1] for v in each], rates[0:1]


def sums_to_send(pairs, even, odd):
    row = lax.broadcasted_iota(jnp.int32, (8, LANES), 0)
    group = lax.broadcasted_iota(jnp.int32, (8, LANES), 1) // (LANES // pairs)
    matrix = jnp.zeros((8, LANES), jnp.float32)
    for p in range(pairs):
        for k, part in ((2 * p, even[p]), (2 * p + 1, odd[p])):
            if part is not None:
                matrix = jnp.where(row == k, jnp.sum(part, axis=0, keepdims=True), matrix)
    sums = jnp.sum(matrix, axis=1, keepdims=True)
    return same_parity(jnp.where(group == row // 2, sums, 0.0))


def put_sums(send, sums):
    for start in range(0, send.shape[0], 8):
        send[start : start + 8, :] = sums


def primal_rows(pairs, per, start, count, taus, tau_side, row_mask, sides, price, u, a, b, a_out, b_out, a_far, b_far, sums):
    span, later = pl.ds(start, count), pl.ds(start + 1, count)
    sums = list(sums)
    side_rate = tau_side * sides if row_mask is None else tau_side * sides * row_mask
    masked = taus if row_mask is None else [tau * row_mask for tau in taus]

    def cell(t, p, here, right):
        rate, grad_rate = (tau_side, side_rate) if p is None else (taus[p], masked[p])
        cost = price[per if p is None else t % per, span, :]
        old_down, old_right = a[t, span, :], b[t, span, :]
        down = old_down + grad_rate * (u[t, later, :] - here)
        across = old_right + grad_rate * (right - here)
        square = down * down + across * across
        factor = jnp.maximum(1.0 - (rate * cost) * lax.rsqrt(square), 0.0)
        new_down, new_right = factor * down, factor * across
        a_out[t, span, :] = new_down
        b_out[t, span, :] = new_right
        change_down, change_right = new_down - old_down, new_right - old_right
        a_far[t, span, :] = new_down + change_down
        b_far[t, span, :] = new_right + change_right
        if sums and p is not None:
            sums[p] = sums[p] + folded(change_down * change_down + change_right * change_right)

    from_right(pairs, per, u, start, count, cell)
    return sums


def dual_rows(pairs, per, start, count, sigmas, sigma_side, source, a_far, b_far, u, u_out, sums):
    span, earlier = pl.ds(start, count), pl.ds(start - 1, count)
    sums = list(sums)

    def cell(t, p, here, left):
        spread = a_far[t, span, :] - a_far[t, earlier, :] + (here - left)
        change = (sigma_side if p is None else sigmas[p]) * (spread - source[t, span, :])
        u_out[t, span, :] = u[t, span, :] + change
        if sums and p is not None:
            sums[p] = sums[p] + folded(change * change)

    from_left(pairs, per, b_far, start, count, cell)
    return sums


def iterate_kernel(pairs, rows, sending, recv, rates, price, source, u, a, b, u_out, a_out, b_out, send, rates_out, *rest):
    slabs, (a_far, b_far) = rest[:-2], rest[-2:]
    per = price.shape[0] - 1
    tiles = pairs * per
    end, last = TOP + rows, rows // CHUNK - 1
    rates_now = next_rates(recv, rates)
    rates_out[...] = rates_now
    taus, tau_side, sigmas, sigma_side = spread_rates(pairs, rates_now)
    above, below, sides = own_masks(pairs)
    a_far[:, 0:PAD, :] = jnp.zeros((tiles + 1, PAD, LANES), jnp.float32)
    u_out[:, end + SLAB : end + TOP, :] = jnp.zeros((tiles + 1, PAD, LANES), jnp.float32)

    def primal(start, count, mask, sums):
        return primal_rows(
            pairs, per, start, count, taus, tau_side, mask, sides, price, u, a, b, a_out, b_out, a_far, b_far, sums
        )

    def dual(start, count, mask, sums):
        now = sigmas if mask is None else [sigma * mask for sigma in sigmas]
        side_now = sigma_side * sides if mask is None else sigma_side * sides * mask
        return dual_rows(pairs, per, start, count, now, side_now, source, a_far, b_far, u, u_out, sums)

    zeros = [jnp.zeros((8, LANES), jnp.float32)] * pairs
    primal(PAD, SLAB, above, ())
    dual(PAD, SLAB, above, ())
    primals = primal(TOP, CHUNK, None, zeros)

    def turn(k, carried):
        primals, duals = carried
        start = TOP + k * CHUNK
        primals = primal(start, CHUNK, None, primals)
        duals = dual(start - CHUNK, CHUNK, None, duals)
        return tuple(primals), tuple(duals)

    primals, duals = lax.fori_loop(1, last + 1, turn, (tuple(primals), tuple(zeros)))
    primal(end, SLAB, below, ())
    duals = dual(TOP + last * CHUNK, CHUNK, None, duals)
    dual(end, SLAB, below, ())
    put_sums(send, sums_to_send(pairs, primals, duals))
    if sending:
        up, down = slabs
        for k, out in enumerate((u_out, a_out, b_out)):
            for t in range(tiles + 1):
                up[strip(k * (tiles + 1) + t), :] = out[t, TOP : TOP + DEPTH, :]
                down[strip(k * (tiles + 1) + t), :] = out[t, end - DEPTH : end, :]


def largest_chunk(rows):
    return max(size for size in range(8, 65, 8) if rows % size == 0)


def early_kernel(pairs, rows, price, source, u, a, b, u_out, a_out, b_out, a_far, b_far, sums_out):
    per = price.shape[0] - 1
    tiles, end = pairs * per, TOP + rows
    rates, side = [initial_step] * pairs, jnp.full((1, LANES), initial_step, jnp.float32)
    sides = own_masks(pairs)[2]
    a_far[:, 0:PAD, :] = jnp.zeros((tiles + 1, PAD, LANES), jnp.float32)
    u_out[:, end + SLAB : end + TOP, :] = jnp.zeros((tiles + 1, PAD, LANES), jnp.float32)
    zeros = (jnp.zeros((8, LANES), jnp.float32),) * pairs
    size = largest_chunk(rows - 8)

    def primal_turn(k, sums):
        start = TOP + k * size
        out = (a_out, b_out, a_far, b_far)
        return tuple(primal_rows(pairs, per, start, size, rates, side, None, sides, price, u, a, b, *out, sums))

    primals = lax.fori_loop(0, (rows - 8) // size, primal_turn, zeros)
    step = largest_chunk(rows - 16)

    def dual_turn(k, sums):
        start = TOP + 8 + k * step
        return tuple(dual_rows(pairs, per, start, step, rates, side * sides, source, a_far, b_far, u, u_out, sums))

    duals = lax.fori_loop(0, (rows - 16) // step, dual_turn, zeros)
    for p in range(pairs):
        sums_out[p] = primals[p]
        sums_out[pairs + p] = duals[p]


def late_kernel(pairs, rows, price, source, u, a, b, sums, *refs):
    u_out, a_out, b_out, a_far, b_far, send = refs[5:]
    per, end = price.shape[0] - 1, TOP + rows
    rates, side = [initial_step] * pairs, jnp.full((1, LANES), initial_step, jnp.float32)
    above, below, sides = own_masks(pairs)

    def primal(start, mask, sums):
        out = (a_out, b_out, a_far, b_far)
        return primal_rows(pairs, per, start, 8, rates, side, mask, sides, price, u, a, b, *out, sums)

    def dual(start, mask, sums):
        now, side_now = (rates, side * sides) if mask is None else ([mask * r for r in rates], side * sides * mask)
        return dual_rows(pairs, per, start, 8, now, side_now, source, a_far, b_far, u, u_out, sums)

    primal(PAD, above, ())
    primals = primal(end - 8, None, [sums[p] for p in range(pairs)])
    primal(end, below, ())
    duals = dual(TOP, None, [sums[pairs + p] for p in range(pairs)])
    duals = dual(end - 8, None, duals)
    dual(PAD, above, ())
    dual(end, below, ())
    put_sums(send, sums_to_send(pairs, primals, duals))


def merge_kernel(rows, recv, top, bottom, u, a, b, u_out, a_out, b_out):
    tiles = u.shape[0]
    for k, out in enumerate((u_out, a_out, b_out)):
        for t in range(tiles):
            out[t, TOP - DEPTH : TOP, :] = top[strip(k * tiles + t), :]
            out[t, TOP + rows : TOP + rows + DEPTH, :] = bottom[strip(k * tiles + t), :]


def closing_kernel(
    pairs, recv, rates, price, source, u, a, b, flow_out, pot_out, send, a_new, b_new, a_far, b_far
):
    per = price.shape[0] - 1
    rows = pot_out.shape[1]
    taus, tau_side, sigmas, _ = spread_rates(pairs, next_rates(recv, rates))
    above, _, sides = own_masks(pairs)

    def primal(start, count, mask):
        primal_rows(
            pairs, per, start, count, taus, tau_side, mask, sides, price, u, a, b, a_new, b_new, a_far, b_far, ()
        )

    def close(k, sums):
        sums = list(sums)
        start = TOP + k * CLOSING_CHUNK
        span, earlier, own = pl.ds(start, CLOSING_CHUNK), pl.ds(start - 1, CLOSING_CHUNK), pl.ds(k * CLOSING_CHUNK, CLOSING_CHUNK)

        def lanes(t):
            return slice(t % per * LANES, (t % per + 1) * LANES)

        def shortfall(t, p, here, left):
            down = a_new[t, span, :]
            missing = down - a_new[t, earlier, :] + (here - left) - source[t, span, :]
            flow_out[0, p, own, lanes(t)] = down
            flow_out[1, p, own, lanes(t)] = here
            sums[p] = sums[p] + folded(missing * missing)

        def rise(t, p, here, left):
            spread = a_far[t, span, :] - a_far[t, earlier, :] + (here - left)
            pot_out[p, own, lanes(t)] = u[t, span, :] + sigmas[p] * (spread - source[t, span, :])

        from_left(pairs, per, b_new, start, CLOSING_CHUNK, shortfall, closing=True)
        from_left(pairs, per, b_far, start, CLOSING_CHUNK, rise, closing=True)
        return tuple(sums)

    primal(PAD, SLAB, above)
    primal(TOP, CLOSING_CHUNK, None)

    def turn(k, sums):
        primal(TOP + k * CLOSING_CHUNK, CLOSING_CHUNK, None)
        return close(k - 1, sums)

    last = rows // CLOSING_CHUNK - 1
    short = lax.fori_loop(1, last + 1, turn, (jnp.zeros((8, LANES), jnp.float32),) * pairs)
    short = close(last, short)
    put_sums(send, sums_to_send(pairs, short, [None] * pairs))


def call(kernel, out_shape, operands, aliases=None, scratch=(), limit=8, space=pltpu.VMEM, flops=0):
    vmem = pl.BlockSpec(memory_space=pltpu.VMEM)
    return pl.pallas_call(
        kernel,
        out_shape=out_shape,
        in_specs=[pl.BlockSpec(memory_space=space)] * len(operands),
        out_specs=[vmem] * len(out_shape),
        input_output_aliases=aliases or {},
        scratch_shapes=list(scratch),
        cost_estimate=pl.CostEstimate(flops=flops, bytes_accessed=0, transcendentals=0) if flops else None,
        compiler_params=pltpu.CompilerParams(vmem_limit_bytes=limit << 20),
    )(*operands)


def kept(*dims):
    return pltpu.VMEM(dims, jnp.float32)


def exchange(send):
    return lax.all_to_all(send, AXES, 0, 0, tiled=True)


def local(imbalance, flow, potential, cost):
    pairs, rows, cols = imbalance.shape
    per = cols // LANES
    tiles = pairs * per
    height = rows + 2 * TOP
    devices = lax.axis_size("gy") * lax.axis_size("gx")

    arrays, count = 4 * pairs + 1, 4 * tiles + per
    edge = kept(5, rows, LANES)
    inputs = [imbalance, flow, potential, cost]
    held = [pltpu.with_memory_space_constraint(x, pltpu.MemorySpace.HBM) for x in inputs]
    sems = pltpu.SemaphoreType.DMA((10,))
    left, right = call(
        functools.partial(edge_columns_kernel, pairs),
        [edge, edge],
        held,
        scratch=[kept(arrays, rows, LANES)] * 2 + [sems],
        space=pltpu.MemorySpace.HBM,
    )
    own_up, own_down = call(
        functools.partial(edge_rows_kernel, pairs),
        [strips(count), strips(count)],
        held,
        scratch=[kept(arrays, SLAB, cols)] * 2 + [sems],
        space=pltpu.MemorySpace.HBM,
        flops=20_000_000,
    )
    left, right = neighbour(left, "gx", -1), neighbour(right, "gx", 1)
    up, down = call(
        functools.partial(slab_kernel, rows, count), [strips(count + 5)] * 2, [left, right, own_up, own_down]
    )
    bottom, top = neighbour(up, "gy", -1), neighbour(down, "gy", 1)

    field = kept(tiles + 1, height, LANES)
    fields = [field] * 4 + [kept(per + 1, height, LANES)]
    started = call(functools.partial(assemble_kernel, pairs), fields, inputs + [left, right], flops=40_000_000)
    u, a, b, source, price = started
    *early, early_sums = call(
        functools.partial(early_kernel, pairs, rows),
        [field] * 5 + [kept(2 * pairs, 8, LANES)],
        [price, source, u, a, b],
        flops=100_000_000,
    )
    u, a, b, source, price = call(
        functools.partial(adopt_kernel, pairs, rows),
        fields,
        [early_sums, top, bottom, *started],
        aliases={k + 3: k for k in range(5)},
    )
    u, a, b, _, _, send = call(
        functools.partial(late_kernel, pairs, rows),
        [field] * 5 + [kept(2 * devices, LANES)],
        [price, source, u, a, b, early_sums, *early],
        aliases={k + 6: k for k in range(5)},
    )
    recv = exchange(send)
    rates = jnp.full((8, LANES), initial_step, jnp.float32)
    for k in range(2, ITERS):
        sending = k % DEPTH == 0
        u, a, b, send, rates, *slabs = call(
            functools.partial(iterate_kernel, pairs, rows, sending),
            [field] * 3 + [kept(2 * devices, LANES), kept(8, LANES)] + [strips(3 * (tiles + 1))] * 2 * sending,
            [recv, rates, price, source, u, a, b],
            scratch=[field] * 2,
        )
        if sending:
            bottom, top = neighbour(slabs[0], "gy", -1), neighbour(slabs[1], "gy", 1)
        recv = exchange(send)
        if sending:
            u, a, b = call(
                functools.partial(merge_kernel, rows),
                [field] * 3,
                [recv, top, bottom, u, a, b],
                aliases={3: 0, 4: 1, 5: 2},
            )
    flow_out, pot_out, send = call(
        functools.partial(closing_kernel, pairs),
        [kept(2, pairs, rows, cols), kept(pairs, rows, cols), kept(2 * devices, LANES)],
        [recv, rates, price, source, u, a, b],
        scratch=[field] * 4,
        limit=12,
    )
    cells = rows * lax.axis_size("gy") * cols * lax.axis_size("gx")
    residual = jnp.sum(exchange(send), axis=0)[:: LANES // pairs] / cells
    return flow_out, pot_out, residual


def solution(mesh):
    placed = (P(None, "gy", "gx"), P(None, None, "gy", "gx"), P(None, "gy", "gx"), P("gy", "gx"))
    return jax.shard_map(
        local,
        mesh=mesh,
        in_specs=placed,
        out_specs=(P(None, None, "gy", "gx"), P(None, "gy", "gx"), P()),
        check_vma=False,
    )
```

```python
import functools

import jax
import jax.numpy as jnp
from jax import lax
from jax.experimental import pallas as pl
from jax.experimental.pallas import tpu as pltpu
from jax.sharding import PartitionSpec as P

ITERS = 12
initial_step = 0.35
epsilon = 1e-06

DEPTH = 6
SIDE = ITERS
SLAB = 8
PAD = 8
TOP = PAD + SLAB
LANES = 128
CLOSING_CHUNK = 64
CHUNK = 32
AXES = ("gy", "gx")


def neighbour(value, axis, steps):
    count = lax.axis_size(axis)
    leading, last = (max(0, -steps), min(count, count - steps))
    return lax.ppermute(value, axis, [(source, source + steps) for source in range(leading, last)])


def rolled(value, shift):
    shift = shift % LANES
    return pltpu.roll(value, shift, 1) if shift else value


def edge_columns_kernel(pairs, imb, flow, pot, cost, left, right, first, last, sems):
    rows, cols = cost.shape
    group = LANES // pairs
    fields = [pot, flow.at[0], flow.at[1], imb]
    copies = []

    def fetch(source, target):
        copies.append(pltpu.make_async_copy(source, target, sems.at[len(copies)]))

    for k, field in enumerate(fields):
        fetch(field.at[:, :, 0:LANES], first.at[pl.ds(k * pairs, pairs)])
        fetch(field.at[:, :, cols - LANES : cols], last.at[pl.ds(k * pairs, pairs)])
    fetch(cost.at[:, 0:LANES], first.at[4 * pairs])
    fetch(cost.at[:, cols - LANES : cols], last.at[4 * pairs])
    for copy in copies:
        copy.start()
    count = 32
    lane = lax.broadcasted_iota(jnp.int32, (count, LANES), 1)
    inner, which = lane % group, lane // group
    for k in range(5):
        for copy in copies[2 * k : 2 * k + 2]:
            copy.wait()
        for start in range(0, rows, count):
            span = slice(start, start + count)
            head = jnp.zeros((count, LANES), jnp.float32)
            tail = jnp.zeros((count, LANES), jnp.float32)
            for p in range(pairs):
                n = min(k * pairs + p, 4 * pairs)
                head = jnp.where((which == p) & (inner < SIDE), rolled(first[n, span, :], group * p), head)
                tail = jnp.where((which == p) & (inner >= group - SIDE), rolled(last[n, span, :], group * (p + 1)), tail)
            left[k, span, :] = head
            right[k, span, :] = tail


def edge_rows_kernel(pairs, imb, flow, pot, cost, up, down, top, bottom, sems):
    rows, cols = cost.shape
    per = cols // LANES
    copies = []

    def fetch(source, target):
        copies.append(pltpu.make_async_copy(source, target, sems.at[len(copies)]))

    for k, field in enumerate([pot, flow.at[0], flow.at[1], imb]):
        fetch(field.at[:, 0:SLAB, :], top.at[pl.ds(k * pairs, pairs)])
        fetch(field.at[:, rows - SLAB : rows, :], bottom.at[pl.ds(k * pairs, pairs)])
    fetch(cost.at[0:SLAB, :], top.at[4 * pairs])
    fetch(cost.at[rows - SLAB : rows, :], bottom.at[4 * pairs])
    for copy in copies:
        copy.start()
    for copy in copies:
        copy.wait()
    for n in range(4 * pairs + 1):
        for c in range(per):
            span = slice(c * LANES, (c + 1) * LANES)
            up[strip(n * per + c), :] = top[n, 0:DEPTH, span]
            down[strip(n * per + c), :] = bottom[n, SLAB - DEPTH : SLAB, span]


def strip(n):
    return slice(n * DEPTH, (n + 1) * DEPTH)


def strips(count):
    return kept(-(-count * DEPTH // 8) * 8, LANES)


def slab_kernel(rows, count, left, right, own_up, own_down, up, down):
    up[0 : count * DEPTH, :] = own_up[0 : count * DEPTH, :]
    down[0 : count * DEPTH, :] = own_down[0 : count * DEPTH, :]
    for k in range(5):
        up[strip(count + k), :] = left[k, 0:DEPTH, :] + right[k, 0:DEPTH, :]
        down[strip(count + k), :] = left[k, rows - DEPTH : rows, :] + right[k, rows - DEPTH : rows, :]


def own_masks(pairs):
    gy, gx = lax.axis_index("gy"), lax.axis_index("gx")
    above = jnp.where(gy > 0, 1.0, 0.0).astype(jnp.float32)
    below = jnp.where(gy < lax.axis_size("gy") - 1, 1.0, 0.0).astype(jnp.float32)
    inner = lax.broadcasted_iota(jnp.int32, (1, LANES), 1) % (LANES // pairs)
    to_right = (inner < SIDE) & (gx < lax.axis_size("gx") - 1)
    to_left = (inner >= LANES // pairs - SIDE) & (gx > 0)
    sides = jnp.where(to_right | to_left, 1.0, 0.0).astype(jnp.float32)
    return above, below, sides


def assemble_kernel(pairs, imb, flow, pot, cost, left, right, u, a, b, source, price):
    rows, cols = cost.shape
    per = cols // LANES
    tiles = pairs * per
    end = TOP + rows
    fields = [(u, pot), (a, flow.at[0]), (b, flow.at[1]), (source, imb)]
    blank = jnp.zeros((tiles + 1, TOP, LANES), jnp.float32)
    for k, (into, field) in enumerate(fields):
        into[:, 0:TOP, :] = blank
        into[:, end : end + TOP, :] = blank
        for p in range(pairs):
            for c in range(per):
                into[p * per + c, TOP:end, :] = field[p, :, c * LANES : (c + 1) * LANES]
        into[tiles, TOP:end, :] = left[k] + right[k]
    sides = own_masks(pairs)[2]
    price[:, 0:TOP, :] = jnp.ones((per + 1, TOP, LANES), jnp.float32)
    price[:, end : end + TOP, :] = jnp.ones((per + 1, TOP, LANES), jnp.float32)
    for c in range(per):
        price[c, TOP:end, :] = cost[:, c * LANES : (c + 1) * LANES]
    price[per, TOP:end, :] = jnp.where(sides > 0.0, left[4] + right[4], 1.0)


def adopt_kernel(pairs, rows, early_sums, top, bottom, u, a, b, source, price, u_out, a_out, b_out, source_out, price_out):
    per = price.shape[0] - 1
    tiles = pairs * per
    end, count = TOP + rows, 4 * tiles + per
    above, below, sides = own_masks(pairs)
    for span, slab, mask in ((slice(TOP - DEPTH, TOP), top, above), (slice(end, end + DEPTH), bottom, below)):
        for k, out in enumerate((u_out, a_out, b_out, source_out)):
            for t in range(tiles):
                out[t, span, :] = slab[strip(k * tiles + t), :]
            out[tiles, span, :] = slab[strip(count + k), :]
        for c in range(per):
            price_out[c, span, :] = slab[strip(4 * tiles + c), :] + (1.0 - mask)
        price_out[per, span, :] = jnp.where(sides * mask > 0.0, slab[strip(count + 4), :], 1.0)


def from_left(pairs, per, b, start, count, cell, closing=False):
    group, tiles = LANES // pairs, pairs * per
    span = pl.ds(start, count)
    lane = lax.broadcasted_iota(jnp.int32, (count, LANES), 1)
    side = b[tiles, span, :]
    moved_side = rolled(side, 1)
    for p in range(pairs):
        before = rolled(side, -(group * p + group - 1))
        for c in range(per):
            here = b[p * per + c, span, :]
            moved = rolled(here, 1)
            cell(p * per + c, p, here, jnp.where(lane == 0, before, moved))
            before = moved
        if not closing:
            moved_side = jnp.where(lane == group * p, rolled(before, group * p), moved_side)
    if not closing:
        cell(tiles, None, side, moved_side)


def from_right(pairs, per, u, start, count, cell):
    group, tiles = LANES // pairs, pairs * per
    span = pl.ds(start, count)
    lane = lax.broadcasted_iota(jnp.int32, (count, LANES), 1)
    side = u[tiles, span, :]
    moved_side = rolled(side, -1)
    for p in range(pairs):
        after = rolled(side, -1 - group * p)
        for c in reversed(range(per)):
            here = u[p * per + c, span, :]
            moved = rolled(here, -1)
            cell(p * per + c, p, here, jnp.where(lane == LANES - 1, after, moved))
            after = moved
        moved_side = jnp.where(lane == group * p + group - 1, rolled(after, group * p + group), moved_side)
    cell(tiles, None, side, moved_side)


def folded(value):
    return jnp.sum(value.reshape(-1, 8, LANES), axis=0)


def row_lanes(pairs):
    assert 2 * pairs == 8
    return lax.broadcasted_iota(jnp.int32, (8, LANES), 0) == lax.broadcasted_iota(jnp.int32, (8, LANES), 1)


def next_rates(pairs, recv, rates):
    total = jnp.sum(folded(recv[...]), axis=0, keepdims=True)
    each = jnp.sum(jnp.where(row_lanes(pairs), total, 0.0), axis=1, keepdims=True) + epsilon
    each = jnp.broadcast_to(each, (8, LANES))
    return rates[...] * lax.rsqrt(lax.rsqrt(each / pltpu.roll(each, pairs, 0)))


def spread_rates(pairs, rates):
    group = lax.broadcasted_iota(jnp.int32, (1, LANES), 1) // (LANES // pairs)
    out = []
    for first in (pairs, 0):
        each = [rates[first + p : first + p + 1] for p in range(pairs)]
        side = each[0]
        for p in range(1, pairs):
            side = jnp.where(group == p, each[p], side)
        out += [each, side]
    return out


def sums_to_send(pairs, primals, duals):
    row = lax.broadcasted_iota(jnp.int32, (8, LANES), 0)
    matrix = jnp.zeros((8, LANES), jnp.float32)
    for k, part in enumerate([*primals, *duals]):
        matrix = jnp.where(row == k, jnp.sum(part, axis=0, keepdims=True), matrix)
    sums = jnp.sum(matrix, axis=1, keepdims=True)
    line = jnp.sum(jnp.where(row_lanes(pairs), sums, 0.0), axis=0, keepdims=True)
    return jnp.broadcast_to(line, (8, LANES))


def put_sums(send, sums):
    for start in range(0, send.shape[0], 8):
        send[start : start + 8, :] = sums


def primal_rows(pairs, per, start, count, taus, tau_side, row_mask, sides, price, u, a, b, a_out, b_out, a_far, b_far, sums):
    span, later = pl.ds(start, count), pl.ds(start + 1, count)
    sums = list(sums)
    side_rate = tau_side * sides if row_mask is None else tau_side * sides * row_mask
    masked = taus if row_mask is None else [tau * row_mask for tau in taus]

    def cell(t, p, here, right):
        rate, grad_rate = (tau_side, side_rate) if p is None else (taus[p], masked[p])
        cost = price[per if p is None else t % per, span, :]
        old_down, old_right = a[t, span, :], b[t, span, :]
        down = old_down + grad_rate * (u[t, later, :] - here)
        across = old_right + grad_rate * (right - here)
        square = down * down + across * across
        factor = jnp.maximum(1.0 - (rate * cost) * lax.rsqrt(square), 0.0)
        new_down, new_right = factor * down, factor * across
        a_out[t, span, :] = new_down
        b_out[t, span, :] = new_right
        change_down, change_right = new_down - old_down, new_right - old_right
        a_far[t, span, :] = new_down + change_down
        b_far[t, span, :] = new_right + change_right
        if sums and p is not None:
            sums[p] = sums[p] + folded(change_down * change_down + change_right * change_right)

    from_right(pairs, per, u, start, count, cell)
    return sums


def dual_rows(pairs, per, start, count, sigmas, sigma_side, source, a_far, b_far, u, u_out, sums):
    span, earlier = pl.ds(start, count), pl.ds(start - 1, count)
    sums = list(sums)

    def cell(t, p, here, left):
        spread = a_far[t, span, :] - a_far[t, earlier, :] + (here - left)
        change = (sigma_side if p is None else sigmas[p]) * (spread - source[t, span, :])
        u_out[t, span, :] = u[t, span, :] + change
        if sums and p is not None:
            sums[p] = sums[p] + folded(change * change)

    from_left(pairs, per, b_far, start, count, cell)
    return sums


def iterate_kernel(pairs, rows, sending, recv, rates, price, source, u, a, b, u_out, a_out, b_out, send, rates_out, *rest):
    slabs, (a_far, b_far) = rest[:-2], rest[-2:]
    per = price.shape[0] - 1
    tiles = pairs * per
    end, last = TOP + rows, rows // CHUNK - 1
    rates_now = next_rates(pairs, recv, rates)
    rates_out[...] = rates_now
    taus, tau_side, sigmas, sigma_side = spread_rates(pairs, rates_now)
    above, below, sides = own_masks(pairs)
    a_far[:, 0:PAD, :] = jnp.zeros((tiles + 1, PAD, LANES), jnp.float32)
    u_out[:, end + SLAB : end + TOP, :] = jnp.zeros((tiles + 1, PAD, LANES), jnp.float32)

    def primal(start, count, mask, sums):
        return primal_rows(
            pairs, per, start, count, taus, tau_side, mask, sides, price, u, a, b, a_out, b_out, a_far, b_far, sums
        )

    def dual(start, count, mask, sums):
        now = sigmas if mask is None else [sigma * mask for sigma in sigmas]
        side_now = sigma_side * sides if mask is None else sigma_side * sides * mask
        return dual_rows(pairs, per, start, count, now, side_now, source, a_far, b_far, u, u_out, sums)

    zeros = [jnp.zeros((8, LANES), jnp.float32)] * pairs
    primal(PAD, SLAB, above, ())
    dual(PAD, SLAB, above, ())
    primals = primal(TOP, CHUNK, None, zeros)

    def turn(k, carried):
        primals, duals = carried
        start = TOP + k * CHUNK
        primals = primal(start, CHUNK, None, primals)
        duals = dual(start - CHUNK, CHUNK, None, duals)
        return tuple(primals), tuple(duals)

    primals, duals = lax.fori_loop(1, last + 1, turn, (tuple(primals), tuple(zeros)))
    primal(end, SLAB, below, ())
    duals = dual(TOP + last * CHUNK, CHUNK, None, duals)
    dual(end, SLAB, below, ())
    put_sums(send, sums_to_send(pairs, primals, duals))
    if sending:
        up, down = slabs
        for k, out in enumerate((u_out, a_out, b_out)):
            for t in range(tiles + 1):
                up[strip(k * (tiles + 1) + t), :] = out[t, TOP : TOP + DEPTH, :]
                down[strip(k * (tiles + 1) + t), :] = out[t, end - DEPTH : end, :]


def largest_chunk(rows):
    return max(size for size in range(8, 65, 8) if rows % size == 0)


def early_kernel(pairs, rows, price, source, u, a, b, u_out, a_out, b_out, a_far, b_far, sums_out):
    per = price.shape[0] - 1
    tiles, end = pairs * per, TOP + rows
    rates, side = [initial_step] * pairs, jnp.full((1, LANES), initial_step, jnp.float32)
    sides = own_masks(pairs)[2]
    a_far[:, 0:PAD, :] = jnp.zeros((tiles + 1, PAD, LANES), jnp.float32)
    u_out[:, end + SLAB : end + TOP, :] = jnp.zeros((tiles + 1, PAD, LANES), jnp.float32)
    zeros = (jnp.zeros((8, LANES), jnp.float32),) * pairs
    size = largest_chunk(rows - 8)

    def primal_turn(k, sums):
        start = TOP + k * size
        out = (a_out, b_out, a_far, b_far)
        return tuple(primal_rows(pairs, per, start, size, rates, side, None, sides, price, u, a, b, *out, sums))

    primals = lax.fori_loop(0, (rows - 8) // size, primal_turn, zeros)
    step = largest_chunk(rows - 16)

    def dual_turn(k, sums):
        start = TOP + 8 + k * step
        return tuple(dual_rows(pairs, per, start, step, rates, side * sides, source, a_far, b_far, u, u_out, sums))

    duals = lax.fori_loop(0, (rows - 16) // step, dual_turn, zeros)
    for p in range(pairs):
        sums_out[p] = primals[p]
        sums_out[pairs + p] = duals[p]


def late_kernel(pairs, rows, price, source, u, a, b, sums, *refs):
    u_out, a_out, b_out, a_far, b_far, send = refs[5:]
    per, end = price.shape[0] - 1, TOP + rows
    rates, side = [initial_step] * pairs, jnp.full((1, LANES), initial_step, jnp.float32)
    above, below, sides = own_masks(pairs)

    def primal(start, mask, sums):
        out = (a_out, b_out, a_far, b_far)
        return primal_rows(pairs, per, start, 8, rates, side, mask, sides, price, u, a, b, *out, sums)

    def dual(start, mask, sums):
        now, side_now = (rates, side * sides) if mask is None else ([mask * r for r in rates], side * sides * mask)
        return dual_rows(pairs, per, start, 8, now, side_now, source, a_far, b_far, u, u_out, sums)

    primal(PAD, above, ())
    primals = primal(end - 8, None, [sums[p] for p in range(pairs)])
    primal(end, below, ())
    duals = dual(TOP, None, [sums[pairs + p] for p in range(pairs)])
    duals = dual(end - 8, None, duals)
    dual(PAD, above, ())
    dual(end, below, ())
    put_sums(send, sums_to_send(pairs, primals, duals))


def merge_kernel(rows, recv, top, bottom, u, a, b, u_out, a_out, b_out):
    tiles = u.shape[0]
    for k, out in enumerate((u_out, a_out, b_out)):
        for t in range(tiles):
            out[t, TOP - DEPTH : TOP, :] = top[strip(k * tiles + t), :]
            out[t, TOP + rows : TOP + rows + DEPTH, :] = bottom[strip(k * tiles + t), :]


def closing_kernel(
    pairs, recv, rates, price, source, u, a, b, flow_out, pot_out, send, a_new, b_new, a_far, b_far
):
    per = price.shape[0] - 1
    rows = pot_out.shape[1]
    taus, tau_side, sigmas, _ = spread_rates(pairs, next_rates(pairs, recv, rates))
    above, _, sides = own_masks(pairs)

    def primal(start, count, mask):
        primal_rows(
            pairs, per, start, count, taus, tau_side, mask, sides, price, u, a, b, a_new, b_new, a_far, b_far, ()
        )

    def close(k, sums):
        sums = list(sums)
        start = TOP + k * CLOSING_CHUNK
        span, earlier, own = pl.ds(start, CLOSING_CHUNK), pl.ds(start - 1, CLOSING_CHUNK), pl.ds(k * CLOSING_CHUNK, CLOSING_CHUNK)

        def lanes(t):
            return slice(t % per * LANES, (t % per + 1) * LANES)

        def shortfall(t, p, here, left):
            down = a_new[t, span, :]
            missing = down - a_new[t, earlier, :] + (here - left) - source[t, span, :]
            flow_out[0, p, own, lanes(t)] = down
            flow_out[1, p, own, lanes(t)] = here
            sums[p] = sums[p] + folded(missing * missing)

        def rise(t, p, here, left):
            spread = a_far[t, span, :] - a_far[t, earlier, :] + (here - left)
            pot_out[p, own, lanes(t)] = u[t, span, :] + sigmas[p] * (spread - source[t, span, :])

        from_left(pairs, per, b_new, start, CLOSING_CHUNK, shortfall, closing=True)
        from_left(pairs, per, b_far, start, CLOSING_CHUNK, rise, closing=True)
        return tuple(sums)

    primal(PAD, SLAB, above)
    primal(TOP, CLOSING_CHUNK, None)

    def turn(k, sums):
        primal(TOP + k * CLOSING_CHUNK, CLOSING_CHUNK, None)
        return close(k - 1, sums)

    last = rows // CLOSING_CHUNK - 1
    short = lax.fori_loop(1, last + 1, turn, (jnp.zeros((8, LANES), jnp.float32),) * pairs)
    short = close(last, short)
    put_sums(send, sums_to_send(pairs, short, ()))


def call(kernel, out_shape, operands, aliases=None, scratch=(), limit=8, space=pltpu.VMEM, flops=0):
    vmem = pl.BlockSpec(memory_space=pltpu.VMEM)
    return pl.pallas_call(
        kernel,
        out_shape=out_shape,
        in_specs=[pl.BlockSpec(memory_space=space)] * len(operands),
        out_specs=[vmem] * len(out_shape),
        input_output_aliases=aliases or {},
        scratch_shapes=list(scratch),
        cost_estimate=pl.CostEstimate(flops=flops, bytes_accessed=0, transcendentals=0) if flops else None,
        compiler_params=pltpu.CompilerParams(vmem_limit_bytes=limit << 20),
    )(*operands)


def kept(*dims):
    return pltpu.VMEM(dims, jnp.float32)


def exchange(send):
    return lax.all_to_all(send, AXES, 0, 0, tiled=True)


def local(imbalance, flow, potential, cost):
    pairs, rows, cols = imbalance.shape
    per = cols // LANES
    tiles = pairs * per
    height = rows + 2 * TOP
    devices = lax.axis_size("gy") * lax.axis_size("gx")

    arrays, count = 4 * pairs + 1, 4 * tiles + per
    edge = kept(5, rows, LANES)
    inputs = [imbalance, flow, potential, cost]
    held = [pltpu.with_memory_space_constraint(x, pltpu.MemorySpace.HBM) for x in inputs]
    sems = pltpu.SemaphoreType.DMA((10,))
    left, right = call(
        functools.partial(edge_columns_kernel, pairs),
        [edge, edge],
        held,
        scratch=[kept(arrays, rows, LANES)] * 2 + [sems],
        space=pltpu.MemorySpace.HBM,
    )
    own_up, own_down = call(
        functools.partial(edge_rows_kernel, pairs),
        [strips(count), strips(count)],
        held,
        scratch=[kept(arrays, SLAB, cols)] * 2 + [sems],
        space=pltpu.MemorySpace.HBM,
        flops=20_000_000,
    )
    left, right = neighbour(left, "gx", -1), neighbour(right, "gx", 1)
    up, down = call(
        functools.partial(slab_kernel, rows, count), [strips(count + 5)] * 2, [left, right, own_up, own_down]
    )
    bottom, top = neighbour(up, "gy", -1), neighbour(down, "gy", 1)

    field = kept(tiles + 1, height, LANES)
    fields = [field] * 4 + [kept(per + 1, height, LANES)]
    started = call(functools.partial(assemble_kernel, pairs), fields, inputs + [left, right], flops=40_000_000)
    u, a, b, source, price = started
    *early, early_sums = call(
        functools.partial(early_kernel, pairs, rows),
        [field] * 5 + [kept(2 * pairs, 8, LANES)],
        [price, source, u, a, b],
        flops=100_000_000,
    )
    u, a, b, source, price = call(
        functools.partial(adopt_kernel, pairs, rows),
        fields,
        [early_sums, top, bottom, *started],
        aliases={k + 3: k for k in range(5)},
    )
    u, a, b, _, _, send = call(
        functools.partial(late_kernel, pairs, rows),
        [field] * 5 + [kept(devices, LANES)],
        [price, source, u, a, b, early_sums, *early],
        aliases={k + 6: k for k in range(5)},
    )
    recv = exchange(send)
    rates = jnp.full((8, LANES), initial_step, jnp.float32)
    for k in range(2, ITERS):
        sending = k % DEPTH == 0
        u, a, b, send, rates, *slabs = call(
            functools.partial(iterate_kernel, pairs, rows, sending),
            [field] * 3 + [kept(devices, LANES), kept(8, LANES)] + [strips(3 * (tiles + 1))] * 2 * sending,
            [recv, rates, price, source, u, a, b],
            scratch=[field] * 2,
        )
        if sending:
            bottom, top = neighbour(slabs[0], "gy", -1), neighbour(slabs[1], "gy", 1)
        recv = exchange(send)
        if sending:
            u, a, b = call(
                functools.partial(merge_kernel, rows),
                [field] * 3,
                [recv, top, bottom, u, a, b],
                aliases={3: 0, 4: 1, 5: 2},
            )
    flow_out, pot_out, send = call(
        functools.partial(closing_kernel, pairs),
        [kept(2, pairs, rows, cols), kept(pairs, rows, cols), kept(devices, LANES)],
        [recv, rates, price, source, u, a, b],
        scratch=[field] * 4,
        limit=12,
    )
    cells = rows * lax.axis_size("gy") * cols * lax.axis_size("gx")
    residual = jnp.sum(exchange(send), axis=0)[:pairs] / cells
    return flow_out, pot_out, residual


def solution(mesh):
    placed = (P(None, "gy", "gx"), P(None, None, "gy", "gx"), P(None, "gy", "gx"), P("gy", "gx"))
    return jax.shard_map(
        local,
        mesh=mesh,
        in_specs=placed,
        out_specs=(P(None, None, "gy", "gx"), P(None, "gy", "gx"), P()),
        check_vma=False,
    )
```

```python
import functools

import jax
import jax.numpy as jnp
from jax import lax
from jax.experimental import pallas as pl
from jax.experimental.pallas import tpu as pltpu
from jax.sharding import PartitionSpec as P

ITERS = 12
initial_step = 0.35
epsilon = 1e-06

DEPTH = 6
SIDE = ITERS
SLAB = 8
PAD = 8
TOP = PAD + SLAB
LANES = 128
CLOSING_CHUNK = 128
CHUNK = 32
AXES = ("gy", "gx")


def neighbour(value, axis, steps):
    count = lax.axis_size(axis)
    leading, last = (max(0, -steps), min(count, count - steps))
    return lax.ppermute(value, axis, [(source, source + steps) for source in range(leading, last)])


def rolled(value, shift):
    shift = shift % LANES
    return pltpu.roll(value, shift, 1) if shift else value


def edge_columns_kernel(pairs, imb, flow, pot, cost, left, right, first, last, sems):
    rows, cols = cost.shape
    group = LANES // pairs
    fields = [pot, flow.at[0], flow.at[1], imb]
    copies = []

    def fetch(source, target):
        copies.append(pltpu.make_async_copy(source, target, sems.at[len(copies)]))

    for k, field in enumerate(fields):
        fetch(field.at[:, :, 0:LANES], first.at[pl.ds(k * pairs, pairs)])
        fetch(field.at[:, :, cols - LANES : cols], last.at[pl.ds(k * pairs, pairs)])
    fetch(cost.at[:, 0:LANES], first.at[4 * pairs])
    fetch(cost.at[:, cols - LANES : cols], last.at[4 * pairs])
    for copy in copies:
        copy.start()
    count = 32
    lane = lax.broadcasted_iota(jnp.int32, (count, LANES), 1)
    inner, which = lane % group, lane // group
    for k in range(5):
        for copy in copies[2 * k : 2 * k + 2]:
            copy.wait()
        for start in range(0, rows, count):
            span = slice(start, start + count)
            head = jnp.zeros((count, LANES), jnp.float32)
            tail = jnp.zeros((count, LANES), jnp.float32)
            for p in range(pairs):
                n = min(k * pairs + p, 4 * pairs)
                head = jnp.where((which == p) & (inner < SIDE), rolled(first[n, span, :], group * p), head)
                tail = jnp.where((which == p) & (inner >= group - SIDE), rolled(last[n, span, :], group * (p + 1)), tail)
            left[k, span, :] = head
            right[k, span, :] = tail


def edge_rows_kernel(pairs, imb, flow, pot, cost, up, down, top, bottom, sems):
    rows, cols = cost.shape
    per = cols // LANES
    copies = []

    def fetch(source, target):
        copies.append(pltpu.make_async_copy(source, target, sems.at[len(copies)]))

    for k, field in enumerate([pot, flow.at[0], flow.at[1], imb]):
        fetch(field.at[:, 0:SLAB, :], top.at[pl.ds(k * pairs, pairs)])
        fetch(field.at[:, rows - SLAB : rows, :], bottom.at[pl.ds(k * pairs, pairs)])
    fetch(cost.at[0:SLAB, :], top.at[4 * pairs])
    fetch(cost.at[rows - SLAB : rows, :], bottom.at[4 * pairs])
    for copy in copies:
        copy.start()
    for copy in copies:
        copy.wait()
    ups, downs = (places(start_depths(pairs * per, per, way)) for way in ("up", "down"))
    for n in range(4 * pairs + 1):
        for c in range(per):
            span = slice(c * LANES, (c + 1) * LANES)
            into, out_of = ups[n * per + c], downs[n * per + c]
            up[into, :] = top[n, 0 : height(into), span]
            down[out_of, :] = bottom[n, SLAB - height(out_of) : SLAB, span]


def start_depths(tiles, per, way):
    less = DEPTH - 1
    fields = [DEPTH, less, less, less, less] if way == "up" else [DEPTH, DEPTH, DEPTH, less, DEPTH]
    return [depth for depth in fields[:4] for _ in range(tiles)] + [fields[4]] * per + fields


def later_depths(tiles, way):
    fields = [DEPTH, DEPTH - 1, DEPTH - 1] if way == "up" else [DEPTH] * 3
    return [depth for depth in fields for _ in range(tiles + 1)]


def places(depths):
    ends = [sum(depths[: n + 1]) for n in range(len(depths))]
    return [slice(end - depth, end) for end, depth in zip(ends, depths)]


def height(place):
    return place.stop - place.start


def strips(depths):
    return kept(-(-sum(depths) // 8) * 8, LANES)


def slab_kernel(rows, tiles, per, left, right, own_up, own_down, up, down):
    for way, own, out in (("up", own_up, up), ("down", own_down, down)):
        spots = places(start_depths(tiles, per, way))
        own_rows = spots[-5].start
        out[0:own_rows, :] = own[0:own_rows, :]
        for k, spot in enumerate(spots[-5:]):
            span = slice(0, height(spot)) if way == "up" else slice(rows - height(spot), rows)
            out[spot, :] = left[k, span, :] + right[k, span, :]


def own_masks(pairs):
    gy, gx = lax.axis_index("gy"), lax.axis_index("gx")
    above = jnp.where(gy > 0, 1.0, 0.0).astype(jnp.float32)
    below = jnp.where(gy < lax.axis_size("gy") - 1, 1.0, 0.0).astype(jnp.float32)
    inner = lax.broadcasted_iota(jnp.int32, (1, LANES), 1) % (LANES // pairs)
    to_right = (inner < SIDE) & (gx < lax.axis_size("gx") - 1)
    to_left = (inner >= LANES // pairs - SIDE) & (gx > 0)
    sides = jnp.where(to_right | to_left, 1.0, 0.0).astype(jnp.float32)
    return above, below, sides


def assemble_kernel(pairs, imb, flow, pot, cost, left, right, u, a, b, source, price):
    rows, cols = cost.shape
    per = cols // LANES
    tiles = pairs * per
    end = TOP + rows
    fields = [(u, pot), (a, flow.at[0]), (b, flow.at[1]), (source, imb)]
    blank = jnp.zeros((tiles + 1, TOP, LANES), jnp.float32)
    for k, (into, field) in enumerate(fields):
        into[:, 0:TOP, :] = blank
        into[:, end : end + TOP, :] = blank
        for p in range(pairs):
            for c in range(per):
                into[p * per + c, TOP:end, :] = field[p, :, c * LANES : (c + 1) * LANES]
        into[tiles, TOP:end, :] = left[k] + right[k]
    sides = own_masks(pairs)[2]
    price[:, 0:TOP, :] = jnp.ones((per + 1, TOP, LANES), jnp.float32)
    price[:, end : end + TOP, :] = jnp.ones((per + 1, TOP, LANES), jnp.float32)
    for c in range(per):
        price[c, TOP:end, :] = cost[:, c * LANES : (c + 1) * LANES]
    price[per, TOP:end, :] = jnp.where(sides > 0.0, left[4] + right[4], 1.0)


def adopt_kernel(pairs, rows, early_sums, top, bottom, u, a, b, source, price, u_out, a_out, b_out, source_out, price_out):
    per = price.shape[0] - 1
    tiles = pairs * per
    end = TOP + rows
    above, below, sides = own_masks(pairs)
    for way, slab, mask in (("down", top, above), ("up", bottom, below)):
        spots = places(start_depths(tiles, per, way))

        def rows_of(spot):
            return slice(TOP - height(spot), TOP) if way == "down" else slice(end, end + height(spot))

        for k, out in enumerate((u_out, a_out, b_out, source_out)):
            for t in range(tiles):
                spot = spots[k * tiles + t]
                out[t, rows_of(spot), :] = slab[spot, :]
            out[tiles, rows_of(spots[-5 + k]), :] = slab[spots[-5 + k], :]
        for c in range(per):
            spot = spots[4 * tiles + c]
            price_out[c, rows_of(spot), :] = slab[spot, :] + (1.0 - mask)
        price_out[per, rows_of(spots[-1]), :] = jnp.where(sides * mask > 0.0, slab[spots[-1], :], 1.0)


def from_left(pairs, per, b, start, count, cell, closing=False):
    group, tiles = LANES // pairs, pairs * per
    span = pl.ds(start, count)
    lane = lax.broadcasted_iota(jnp.int32, (count, LANES), 1)
    side = b[tiles, span, :]
    moved_side = rolled(side, 1)
    for p in range(pairs):
        before = rolled(side, -(group * p + group - 1))
        for c in range(per):
            here = b[p * per + c, span, :]
            moved = rolled(here, 1)
            cell(p * per + c, p, here, jnp.where(lane == 0, before, moved))
            before = moved
        if not closing:
            moved_side = jnp.where(lane == group * p, rolled(before, group * p), moved_side)
    if not closing:
        cell(tiles, None, side, moved_side)


def from_right(pairs, per, u, start, count, cell):
    group, tiles = LANES // pairs, pairs * per
    span = pl.ds(start, count)
    lane = lax.broadcasted_iota(jnp.int32, (count, LANES), 1)
    side = u[tiles, span, :]
    moved_side = rolled(side, -1)
    for p in range(pairs):
        after = rolled(side, -1 - group * p)
        for c in reversed(range(per)):
            here = u[p * per + c, span, :]
            moved = rolled(here, -1)
            cell(p * per + c, p, here, jnp.where(lane == LANES - 1, after, moved))
            after = moved
        moved_side = jnp.where(lane == group * p + group - 1, rolled(after, group * p + group), moved_side)
    cell(tiles, None, side, moved_side)


def folded(value):
    return jnp.sum(value.reshape(-1, 8, LANES), axis=0)


def row_lanes(pairs):
    assert 2 * pairs == 8
    return lax.broadcasted_iota(jnp.int32, (8, LANES), 0) == lax.broadcasted_iota(jnp.int32, (8, LANES), 1)


def next_rates(pairs, recv, rates):
    total = jnp.sum(folded(recv[...]), axis=0, keepdims=True)
    each = jnp.sum(jnp.where(row_lanes(pairs), total, 0.0), axis=1, keepdims=True) + epsilon
    each = jnp.broadcast_to(each, (8, LANES))
    return rates[...] * lax.rsqrt(lax.rsqrt(each / pltpu.roll(each, pairs, 0)))


def spread_rates(pairs, rates):
    group = lax.broadcasted_iota(jnp.int32, (1, LANES), 1) // (LANES // pairs)
    out = []
    for first in (pairs, 0):
        each = [rates[first + p : first + p + 1] for p in range(pairs)]
        side = each[0]
        for p in range(1, pairs):
            side = jnp.where(group == p, each[p], side)
        out += [each, side]
    return out


def sums_to_send(pairs, primals, duals):
    row = lax.broadcasted_iota(jnp.int32, (8, LANES), 0)
    matrix = jnp.zeros((8, LANES), jnp.float32)
    for k, part in enumerate([*primals, *duals]):
        matrix = jnp.where(row == k, jnp.sum(part, axis=0, keepdims=True), matrix)
    sums = jnp.sum(matrix, axis=1, keepdims=True)
    line = jnp.sum(jnp.where(row_lanes(pairs), sums, 0.0), axis=0, keepdims=True)
    return jnp.broadcast_to(line, (8, LANES))


def put_sums(send, sums):
    for start in range(0, send.shape[0], 8):
        send[start : start + 8, :] = sums


def primal_rows(pairs, per, start, count, taus, tau_side, row_mask, sides, price, u, a, b, a_out, b_out, a_far, b_far, sums):
    span, later = pl.ds(start, count), pl.ds(start + 1, count)
    sums = list(sums)
    side_rate = tau_side * sides if row_mask is None else tau_side * sides * row_mask
    masked = taus if row_mask is None else [tau * row_mask for tau in taus]

    def cell(t, p, here, right):
        rate, grad_rate = (tau_side, side_rate) if p is None else (taus[p], masked[p])
        cost = price[per if p is None else t % per, span, :]
        old_down, old_right = a[t, span, :], b[t, span, :]
        down = old_down + grad_rate * (u[t, later, :] - here)
        across = old_right + grad_rate * (right - here)
        square = down * down + across * across
        factor = jnp.maximum(1.0 - (rate * cost) * lax.rsqrt(square), 0.0)
        new_down, new_right = factor * down, factor * across
        a_out[t, span, :] = new_down
        b_out[t, span, :] = new_right
        change_down, change_right = new_down - old_down, new_right - old_right
        a_far[t, span, :] = new_down + change_down
        b_far[t, span, :] = new_right + change_right
        if sums and p is not None:
            sums[p] = sums[p] + folded(change_down * change_down + change_right * change_right)

    from_right(pairs, per, u, start, count, cell)
    return sums


def dual_rows(pairs, per, start, count, sigmas, sigma_side, source, a_far, b_far, u, u_out, sums):
    span, earlier = pl.ds(start, count), pl.ds(start - 1, count)
    sums = list(sums)

    def cell(t, p, here, left):
        spread = a_far[t, span, :] - a_far[t, earlier, :] + (here - left)
        change = (sigma_side if p is None else sigmas[p]) * (spread - source[t, span, :])
        u_out[t, span, :] = u[t, span, :] + change
        if sums and p is not None:
            sums[p] = sums[p] + folded(change * change)

    from_left(pairs, per, b_far, start, count, cell)
    return sums


def iterate_kernel(pairs, rows, sending, recv, rates, price, source, u, a, b, u_out, a_out, b_out, send, rates_out, *rest):
    slabs, (a_far, b_far) = rest[:-2], rest[-2:]
    per = price.shape[0] - 1
    tiles = pairs * per
    end, last = TOP + rows, rows // CHUNK - 1
    rates_now = next_rates(pairs, recv, rates)
    rates_out[...] = rates_now
    taus, tau_side, sigmas, sigma_side = spread_rates(pairs, rates_now)
    above, below, sides = own_masks(pairs)
    a_far[:, 0:PAD, :] = jnp.zeros((tiles + 1, PAD, LANES), jnp.float32)
    u_out[:, end + SLAB : end + TOP, :] = jnp.zeros((tiles + 1, PAD, LANES), jnp.float32)

    def primal(start, count, mask, sums):
        return primal_rows(
            pairs, per, start, count, taus, tau_side, mask, sides, price, u, a, b, a_out, b_out, a_far, b_far, sums
        )

    def dual(start, count, mask, sums):
        now = sigmas if mask is None else [sigma * mask for sigma in sigmas]
        side_now = sigma_side * sides if mask is None else sigma_side * sides * mask
        return dual_rows(pairs, per, start, count, now, side_now, source, a_far, b_far, u, u_out, sums)

    zeros = [jnp.zeros((8, LANES), jnp.float32)] * pairs
    primal(PAD, SLAB, above, ())
    dual(PAD, SLAB, above, ())
    primals = primal(TOP, CHUNK, None, zeros)

    def turn(k, carried):
        primals, duals = carried
        start = TOP + k * CHUNK
        primals = primal(start, CHUNK, None, primals)
        duals = dual(start - CHUNK, CHUNK, None, duals)
        return tuple(primals), tuple(duals)

    primals, duals = lax.fori_loop(1, last + 1, turn, (tuple(primals), tuple(zeros)))
    primal(end, SLAB, below, ())
    duals = dual(TOP + last * CHUNK, CHUNK, None, duals)
    dual(end, SLAB, below, ())
    put_sums(send, sums_to_send(pairs, primals, duals))
    if sending:
        up, down = slabs
        ups, downs = (places(later_depths(tiles, way)) for way in ("up", "down"))
        for k, out in enumerate((u_out, a_out, b_out)):
            for t in range(tiles + 1):
                n = k * (tiles + 1) + t
                up[ups[n], :] = out[t, TOP : TOP + height(ups[n]), :]
                down[downs[n], :] = out[t, end - height(downs[n]) : end, :]


def largest_chunk(rows):
    return max(size for size in range(8, 65, 8) if rows % size == 0)


def early_kernel(pairs, rows, price, source, u, a, b, u_out, a_out, b_out, a_far, b_far, sums_out):
    per = price.shape[0] - 1
    tiles, end = pairs * per, TOP + rows
    rates, side = [initial_step] * pairs, jnp.full((1, LANES), initial_step, jnp.float32)
    sides = own_masks(pairs)[2]
    a_far[:, 0:PAD, :] = jnp.zeros((tiles + 1, PAD, LANES), jnp.float32)
    u_out[:, end + SLAB : end + TOP, :] = jnp.zeros((tiles + 1, PAD, LANES), jnp.float32)
    zeros = (jnp.zeros((8, LANES), jnp.float32),) * pairs
    size = largest_chunk(rows - 8)

    def primal_turn(k, sums):
        start = TOP + k * size
        out = (a_out, b_out, a_far, b_far)
        return tuple(primal_rows(pairs, per, start, size, rates, side, None, sides, price, u, a, b, *out, sums))

    primals = lax.fori_loop(0, (rows - 8) // size, primal_turn, zeros)
    step = largest_chunk(rows - 16)

    def dual_turn(k, sums):
        start = TOP + 8 + k * step
        return tuple(dual_rows(pairs, per, start, step, rates, side * sides, source, a_far, b_far, u, u_out, sums))

    duals = lax.fori_loop(0, (rows - 16) // step, dual_turn, zeros)
    for p in range(pairs):
        sums_out[p] = primals[p]
        sums_out[pairs + p] = duals[p]


def late_kernel(pairs, rows, price, source, u, a, b, sums, *refs):
    u_out, a_out, b_out, a_far, b_far, send = refs[5:]
    per, end = price.shape[0] - 1, TOP + rows
    rates, side = [initial_step] * pairs, jnp.full((1, LANES), initial_step, jnp.float32)
    above, below, sides = own_masks(pairs)

    def primal(start, mask, sums):
        out = (a_out, b_out, a_far, b_far)
        return primal_rows(pairs, per, start, 8, rates, side, mask, sides, price, u, a, b, *out, sums)

    def dual(start, mask, sums):
        now, side_now = (rates, side * sides) if mask is None else ([mask * r for r in rates], side * sides * mask)
        return dual_rows(pairs, per, start, 8, now, side_now, source, a_far, b_far, u, u_out, sums)

    primal(PAD, above, ())
    primals = primal(end - 8, None, [sums[p] for p in range(pairs)])
    primal(end, below, ())
    duals = dual(TOP, None, [sums[pairs + p] for p in range(pairs)])
    duals = dual(end - 8, None, duals)
    dual(PAD, above, ())
    dual(end, below, ())
    put_sums(send, sums_to_send(pairs, primals, duals))


def merge_kernel(rows, recv, top, bottom, u, a, b, u_out, a_out, b_out):
    tiles, end = u.shape[0] - 1, TOP + rows
    ups, downs = (places(later_depths(tiles, way)) for way in ("up", "down"))
    for k, out in enumerate((u_out, a_out, b_out)):
        for t in range(tiles + 1):
            n = k * (tiles + 1) + t
            out[t, TOP - height(downs[n]) : TOP, :] = top[downs[n], :]
            out[t, end : end + height(ups[n]), :] = bottom[ups[n], :]


def closing_kernel(
    pairs, recv, rates, price, source, u, a, b, flow_out, pot_out, send, a_new, b_new, a_far, b_far
):
    per = price.shape[0] - 1
    rows = pot_out.shape[1]
    taus, tau_side, sigmas, _ = spread_rates(pairs, next_rates(pairs, recv, rates))
    above, _, sides = own_masks(pairs)

    def primal(start, count, mask):
        primal_rows(
            pairs, per, start, count, taus, tau_side, mask, sides, price, u, a, b, a_new, b_new, a_far, b_far, ()
        )

    def close(k, sums):
        sums = list(sums)
        start = TOP + k * CLOSING_CHUNK
        span, earlier, own = pl.ds(start, CLOSING_CHUNK), pl.ds(start - 1, CLOSING_CHUNK), pl.ds(k * CLOSING_CHUNK, CLOSING_CHUNK)

        def lanes(t):
            return slice(t % per * LANES, (t % per + 1) * LANES)

        def shortfall(t, p, here, left):
            down = a_new[t, span, :]
            missing = down - a_new[t, earlier, :] + (here - left) - source[t, span, :]
            flow_out[0, p, own, lanes(t)] = down
            flow_out[1, p, own, lanes(t)] = here
            sums[p] = sums[p] + folded(missing * missing)

        def rise(t, p, here, left):
            spread = a_far[t, span, :] - a_far[t, earlier, :] + (here - left)
            pot_out[p, own, lanes(t)] = u[t, span, :] + sigmas[p] * (spread - source[t, span, :])

        from_left(pairs, per, b_new, start, CLOSING_CHUNK, shortfall, closing=True)
        from_left(pairs, per, b_far, start, CLOSING_CHUNK, rise, closing=True)
        return tuple(sums)

    primal(PAD, SLAB, above)
    primal(TOP, CLOSING_CHUNK, None)

    def turn(k, sums):
        primal(TOP + k * CLOSING_CHUNK, CLOSING_CHUNK, None)
        return close(k - 1, sums)

    last = rows // CLOSING_CHUNK - 1
    short = lax.fori_loop(1, last + 1, turn, (jnp.zeros((8, LANES), jnp.float32),) * pairs)
    short = close(last, short)
    put_sums(send, sums_to_send(pairs, short, ()))


def call(kernel, out_shape, operands, aliases=None, scratch=(), limit=8, space=pltpu.VMEM, flops=0):
    vmem = pl.BlockSpec(memory_space=pltpu.VMEM)
    return pl.pallas_call(
        kernel,
        out_shape=out_shape,
        in_specs=[pl.BlockSpec(memory_space=space)] * len(operands),
        out_specs=[vmem] * len(out_shape),
        input_output_aliases=aliases or {},
        scratch_shapes=list(scratch),
        cost_estimate=pl.CostEstimate(flops=flops, bytes_accessed=0, transcendentals=0) if flops else None,
        compiler_params=pltpu.CompilerParams(vmem_limit_bytes=limit << 20),
    )(*operands)


def kept(*dims):
    return pltpu.VMEM(dims, jnp.float32)


def exchange(send):
    return lax.all_to_all(send, AXES, 0, 0, tiled=True)


def local(imbalance, flow, potential, cost):
    pairs, rows, cols = imbalance.shape
    per = cols // LANES
    tiles = pairs * per
    total_rows = rows + 2 * TOP
    devices = lax.axis_size("gy") * lax.axis_size("gx")

    arrays = 4 * pairs + 1
    moving = [strips(start_depths(tiles, per, way)) for way in ("up", "down")]
    own = [strips(start_depths(tiles, per, way)[:-5]) for way in ("up", "down")]
    later = [strips(later_depths(tiles, way)) for way in ("up", "down")]
    edge = kept(5, rows, LANES)
    inputs = [imbalance, flow, potential, cost]
    held = [pltpu.with_memory_space_constraint(x, pltpu.MemorySpace.HBM) for x in inputs]
    sems = pltpu.SemaphoreType.DMA((10,))
    left, right = call(
        functools.partial(edge_columns_kernel, pairs),
        [edge, edge],
        held,
        scratch=[kept(arrays, rows, LANES)] * 2 + [sems],
        space=pltpu.MemorySpace.HBM,
    )
    own_up, own_down = call(
        functools.partial(edge_rows_kernel, pairs),
        own,
        held,
        scratch=[kept(arrays, SLAB, cols)] * 2 + [sems],
        space=pltpu.MemorySpace.HBM,
        flops=20_000_000,
    )
    left, right = neighbour(left, "gx", -1), neighbour(right, "gx", 1)
    up, down = call(
        functools.partial(slab_kernel, rows, tiles, per), moving, [left, right, own_up, own_down]
    )
    bottom, top = neighbour(up, "gy", -1), neighbour(down, "gy", 1)

    field = kept(tiles + 1, total_rows, LANES)
    fields = [field] * 4 + [kept(per + 1, total_rows, LANES)]
    started = call(functools.partial(assemble_kernel, pairs), fields, inputs + [left, right], flops=40_000_000)
    u, a, b, source, price = started
    *early, early_sums = call(
        functools.partial(early_kernel, pairs, rows),
        [field] * 5 + [kept(2 * pairs, 8, LANES)],
        [price, source, u, a, b],
        flops=100_000_000,
    )
    u, a, b, source, price = call(
        functools.partial(adopt_kernel, pairs, rows),
        fields,
        [early_sums, top, bottom, *started],
        aliases={k + 3: k for k in range(5)},
    )
    u, a, b, _, _, send = call(
        functools.partial(late_kernel, pairs, rows),
        [field] * 5 + [kept(devices, LANES)],
        [price, source, u, a, b, early_sums, *early],
        aliases={k + 6: k for k in range(5)},
    )
    recv = exchange(send)
    rates = jnp.full((8, LANES), initial_step, jnp.float32)
    for k in range(2, ITERS):
        sending = k % DEPTH == 0
        u, a, b, send, rates, *slabs = call(
            functools.partial(iterate_kernel, pairs, rows, sending),
            [field] * 3 + [kept(devices, LANES), kept(8, LANES)] + later * sending,
            [recv, rates, price, source, u, a, b],
            scratch=[field] * 2,
        )
        if sending:
            bottom, top = neighbour(slabs[0], "gy", -1), neighbour(slabs[1], "gy", 1)
        recv = exchange(send)
        if sending:
            u, a, b = call(
                functools.partial(merge_kernel, rows),
                [field] * 3,
                [recv, top, bottom, u, a, b],
                aliases={3: 0, 4: 1, 5: 2},
            )
    flow_out, pot_out, send = call(
        functools.partial(closing_kernel, pairs),
        [kept(2, pairs, rows, cols), kept(pairs, rows, cols), kept(devices, LANES)],
        [recv, rates, price, source, u, a, b],
        scratch=[field] * 4,
        limit=12,
    )
    cells = rows * lax.axis_size("gy") * cols * lax.axis_size("gx")
    residual = jnp.sum(exchange(send), axis=0)[:pairs] / cells
    return flow_out, pot_out, residual


def solution(mesh):
    placed = (P(None, "gy", "gx"), P(None, None, "gy", "gx"), P(None, "gy", "gx"), P("gy", "gx"))
    return jax.shard_map(
        local,
        mesh=mesh,
        in_specs=placed,
        out_specs=(P(None, None, "gy", "gx"), P(None, "gy", "gx"), P()),
        check_vma=False,
    )
```
